32 devices in a mesh: emb: 32 (over z, y, x, core).
Axes of the slice: x: 2, y: 2, z: 4, core: 2. Of those that a mesh axis runs over, the one named last changes fastest.
Arguments:
- x_start: bfloat16 [65536, 1024], P('emb')
- d_out: bfloat16 [65536, 1024], P('emb')
- token_ids: int32 [2, 65536, 4], P(None, 'emb')
- w_up: bfloat16 [4, 1024, 4096], replicated
- w_down: bfloat16 [4, 4096, 1024], replicated
- w_gate: bfloat16 [2, 1024, 1024], replicated
- w_proj: bfloat16 [2, 1024, 1024], replicated
- tables: bfloat16 [2, 131072, 256], P(None, 'emb')
Outputs:
- output 1: bfloat16 [65536, 1024], P('emb')
- output 2: float32 [2, 131072, 256], P(None, 'emb')
All inputs are finite; a program needn't handle non-finite values.
Results may differ from the reference program's by a relative error of at most 0.0153688.
Values are sent between devices in bfloat16 or wider.
A program may use at most 1 GiB of HBM per device.

```python
import jax
import jax.numpy as jnp
from jax import lax

D = 1024
FF = 4096
HEADS = 4
DH = 256
VH = 131072
LAYERS = 4
TOK = 2048
GROUP = 32
ZIPF_TOP = 16777216
ZIPF_SPAN = 262144
HASH_MUL = 2503

TOKENS = TOK * GROUP
ROWS_DEV = VH // GROUP
CAP = max(8, (4 * TOK * HEADS) // GROUP)
WIDE = HEADS * DH
EPS = 1e-6


def draw_block(key_blk, hot_owner, offset):
    key_perm, key_mix, key_rank = jax.random.split(key_blk, 3)
    spare_slot = jax.random.permutation(key_perm, (GROUP - 1) * CAP)[: TOK * HEADS - CAP]
    spare_owner = spare_slot // CAP
    spare_owner = spare_owner + (spare_owner >= hot_owner).astype(jnp.int32)
    owner_ids = jnp.concatenate([jnp.full((CAP,), hot_owner, jnp.int32), spare_owner.astype(jnp.int32)])
    owner_ids = jax.random.permutation(key_mix, owner_ids)
    uniform_draw = jax.random.randint(key_rank, (TOK * HEADS,), 1, ZIPF_SPAN + 1)
    zipf_rank = ZIPF_TOP // uniform_draw
    local_ids = ((zipf_rank % ROWS_DEV) * HASH_MUL + offset) % ROWS_DEV
    return (owner_ids * ROWS_DEV + local_ids).astype(jnp.int32).reshape(TOK, HEADS)


def draw_table(key_tab, hot_owner, offset):
    dev_keys = jax.random.split(key_tab, GROUP)
    blocks = jax.vmap(draw_block, in_axes=(0, None, None))(dev_keys, hot_owner, offset)
    return blocks.reshape(TOKENS, HEADS)


def draw_ids(key_ids):
    key_hot, key_off, key_tab = jax.random.split(key_ids, 3)
    hot_owner = jax.random.randint(key_hot, (2,), 0, GROUP)
    offset = jax.random.randint(key_off, (2,), 0, ROWS_DEV)
    return jax.vmap(draw_table)(jax.random.split(key_tab, 2), hot_owner, offset).astype(jnp.int32)


def setup_inputs(seed: int = 0) -> dict:
    key_list = jax.random.split(jax.random.key(seed), 8)
    x_start = jax.random.normal(key_list[0], (TOKENS, D), jnp.float32).astype(jnp.bfloat16)
    d_out = jax.random.normal(key_list[1], (TOKENS, D), jnp.float32).astype(jnp.bfloat16)
    token_ids = draw_ids(key_list[2])
    w_up = (jax.random.normal(key_list[3], (LAYERS, D, FF), jnp.float32) * D ** -0.5).astype(jnp.bfloat16)
    w_down = (jax.random.normal(key_list[4], (LAYERS, FF, D), jnp.float32) * (0.5 * FF ** -0.5)).astype(jnp.bfloat16)
    w_gate = (jax.random.normal(key_list[5], (2, D, WIDE), jnp.float32) * D ** -0.5).astype(jnp.bfloat16)
    w_proj = (jax.random.normal(key_list[6], (2, WIDE, D), jnp.float32) * (0.5 * WIDE ** -0.5)).astype(jnp.bfloat16)
    tables = jax.random.normal(key_list[7], (2, VH, DH), jnp.float32).astype(jnp.bfloat16)
    return {'x_start': x_start, 'd_out': d_out, 'token_ids': token_ids, 'w_up': w_up, 'w_down': w_down, 'w_gate': w_gate, 'w_proj': w_proj, 'tables': tables}


def gelu_fn(pre_act):
    return jax.nn.gelu(pre_act, approximate=True)


def gelu_grad(pre_act, cotangent):
    _, pullback = jax.vjp(gelu_fn, pre_act.astype(jnp.float32))
    return pullback(cotangent)[0]


def norm_fwd(x_res):
    x_f = x_res.astype(jnp.float32)
    inv_rms = lax.rsqrt(jnp.mean(x_f * x_f, axis=-1, keepdims=True) + EPS)
    return (x_f * inv_rms).astype(jnp.bfloat16), inv_rms


def norm_bwd(x_res, inv_rms, d_norm):
    x_f = x_res.astype(jnp.float32)
    mean_dot = jnp.mean(x_f * d_norm, axis=-1, keepdims=True)
    return inv_rms * d_norm - x_f * (inv_rms * inv_rms * inv_rms) * mean_dot


def block_pass(block_in, w_up, w_down, w_gate, w_proj, tables):
    x_blk, dy_blk, ids_blk = block_in
    slot_of = {1: 0, LAYERS - 1: 1}
    emb_rows = [tables[which][ids_blk[which]].reshape(TOK, WIDE) for which in range(2)]
    saved_acts = []
    x_cur = x_blk
    for layer_idx in range(LAYERS):
        normed, inv_rms = norm_fwd(x_cur)
        hidden = jnp.dot(normed, w_up[layer_idx], preferred_element_type=jnp.float32).astype(jnp.bfloat16)
        activated = gelu_fn(hidden.astype(jnp.float32)).astype(jnp.bfloat16)
        mlp_out = jnp.dot(activated, w_down[layer_idx], preferred_element_type=jnp.float32).astype(jnp.bfloat16)
        new_res = x_cur.astype(jnp.float32) + mlp_out.astype(jnp.float32)
        gate_saved = None
        if layer_idx in slot_of:
            which = slot_of[layer_idx]
            pre_gate = jnp.dot(normed, w_gate[which], preferred_element_type=jnp.float32).astype(jnp.bfloat16)
            gate_val = gelu_fn(pre_gate.astype(jnp.float32)).astype(jnp.bfloat16)
            mixed_val = (gate_val.astype(jnp.float32) * emb_rows[which].astype(jnp.float32)).astype(jnp.bfloat16)
            proj_out = jnp.dot(mixed_val, w_proj[which], preferred_element_type=jnp.float32).astype(jnp.bfloat16)
            new_res = new_res + proj_out.astype(jnp.float32)
            gate_saved = (pre_gate, gate_val)
        saved_acts.append((x_cur, inv_rms, hidden, gate_saved))
        x_cur = new_res.astype(jnp.bfloat16)
    d_res = dy_blk.astype(jnp.float32)
    pieces = [None, None]
    for layer_idx in reversed(range(1, LAYERS)):
        x_prev, inv_rms, hidden, gate_saved = saved_acts[layer_idx]
        d_low = d_res.astype(jnp.bfloat16)
        if gate_saved is not None:
            which = slot_of[layer_idx]
            pre_gate, gate_val = gate_saved
            d_mix = jnp.dot(d_low, w_proj[which].T, preferred_element_type=jnp.float32)
            pieces[which] = (gate_val.astype(jnp.float32) * d_mix).reshape(TOK, HEADS, DH)
        if layer_idx > 1:
            d_act = jnp.dot(d_low, w_down[layer_idx].T, preferred_element_type=jnp.float32)
            d_hid = gelu_grad(hidden, d_act)
            d_norm = jnp.dot(d_hid.astype(jnp.bfloat16), w_up[layer_idx].T, preferred_element_type=jnp.float32)
            if gate_saved is not None:
                d_gate = gelu_grad(pre_gate, d_mix * emb_rows[which].astype(jnp.float32))
                d_norm = d_norm + jnp.dot(d_gate.astype(jnp.bfloat16), w_gate[which].T, preferred_element_type=jnp.float32)
            d_res = d_res + norm_bwd(x_prev, inv_rms, d_norm)
    return x_cur, jnp.stack(pieces)


def reference(x_start, d_out, token_ids, w_up, w_down, w_gate, w_proj, tables):
    def run_block(block_in):
        return block_pass(block_in, w_up, w_down, w_gate, w_proj, tables)
    ids_blocks = jnp.transpose(token_ids.reshape(2, GROUP, TOK, HEADS), (1, 0, 2, 3))
    x_blocks, grad_rows = lax.map(run_block, (x_start.reshape(GROUP, TOK, D), d_out.reshape(GROUP, TOK, D), ids_blocks))
    d_tables = jnp.stack([jax.ops.segment_sum(grad_rows[:, which].reshape(TOKENS * HEADS, DH), token_ids[which].reshape(TOKENS * HEADS), num_segments=VH) for which in range(2)])
    return x_blocks.reshape(TOKENS, D), d_tables
```

```python
import jax
import jax.numpy as jnp
from jax import lax
from jax.experimental import pallas as pl
from jax.experimental.pallas import tpu as pltpu
from jax.sharding import PartitionSpec as P

EPS = 1e-6
VMEM_LIMIT = 60 * 1024 * 1024
MESH = pl.DeviceIdType.MESH
PLANE = 8
SLOTS = 344
IDW = 1024
UNROLL = 16
STREAMS = 4
ACCS = 4


def gelu_fn(pre_act):
    return jax.nn.gelu(pre_act, approximate=True)


def gelu_grad(pre_act, cotangent):
    _, pullback = jax.vjp(gelu_fn, pre_act.astype(jnp.float32))
    return pullback(cotangent)[0]


def norm_fwd(x_res):
    x_f = x_res.astype(jnp.float32)
    inv_rms = lax.rsqrt(jnp.mean(x_f * x_f, axis=-1, keepdims=True) + EPS)
    return (x_f * inv_rms).astype(jnp.bfloat16), inv_rms


def norm_bwd(x_res, inv_rms, d_norm):
    x_f = x_res.astype(jnp.float32)
    mean_dot = jnp.mean(x_f * d_norm, axis=-1, keepdims=True)
    return inv_rms * d_norm - x_f * (inv_rms * inv_rms * inv_rms) * mean_dot


def local_params():
    return pltpu.CompilerParams(vmem_limit_bytes=VMEM_LIMIT)


def remote_params(cid):
    return pltpu.CompilerParams(vmem_limit_bytes=VMEM_LIMIT, collective_id=cid, has_side_effects=True)


def cost(us, nbytes):
    return pl.CostEstimate(flops=int(us * 10**6), bytes_accessed=nbytes, transcendentals=0)


SMEM_SPEC = pl.BlockSpec(memory_space=pltpu.SMEM)
VMEM_SPEC = pl.BlockSpec(memory_space=pltpu.VMEM)
ANY_SPEC = pl.BlockSpec(memory_space=pl.ANY)


def make_ids(uid, start, count, peak, rnd):
    n_tab, n_tgt = count.shape

    def kernel(uid_ref, start_ref, count_ref, peak_ref, rnd_ref, out_ref):
        shift = rnd_ref[0] * SLOTS
        for t in range(n_tab):
            def tgt(g, c):
                base = jnp.minimum(start_ref[t * n_tgt + g] + shift, uid.shape[1] - SLOTS) + t * uid.shape[1]
                o = (g * n_tab + t) * IDW

                def blk(b, c):
                    for j in range(8):
                        out_ref[o + b * 8 + j] = uid_ref[base + b * 8 + j]
                    return c
                lax.fori_loop(0, SLOTS // 8, blk, 0)
                out_ref[o + IDW - 2] = peak_ref[t]
                out_ref[o + IDW - 1] = jnp.clip(count_ref[t * n_tgt + g] - shift, 0, SLOTS)
                return c
            lax.fori_loop(0, n_tgt, tgt, 0)

    return pl.pallas_call(
        kernel, out_shape=jax.ShapeDtypeStruct((n_tgt * n_tab * IDW,), jnp.int32),
        in_specs=[SMEM_SPEC] * 5, out_specs=SMEM_SPEC, compiler_params=local_params(), name="make_ids",
        cost_estimate=cost(10, 2**18),
    )(uid.reshape(-1), start.reshape(-1), count.reshape(-1), peak, jnp.reshape(rnd, (1,)).astype(jnp.int32))


def owner_gather(ids, table3):
    n_src = ids.shape[0] // IDW

    def kernel(ids_ref, table_ref, out_ref):
        rows = table_ref.shape[0]

        def src(s, c):
            def blk(b, c):
                for j in range(8):
                    r = b * 8 + j
                    out_ref[s * SLOTS + r] = table_ref[ids_ref[s * IDW + r] & (rows - 1)]
                return c
            lax.fori_loop(0, SLOTS // 8, blk, 0)
            return c
        lax.fori_loop(0, n_src, src, 0)

    return pl.pallas_call(
        kernel, out_shape=jax.ShapeDtypeStruct((n_src * SLOTS,) + table3.shape[1:], table3.dtype),
        in_specs=[SMEM_SPEC, VMEM_SPEC], out_specs=VMEM_SPEC, compiler_params=local_params(), name="owner_gather",
        cost_estimate=cost(10, 2**22),
    )(ids, table3)


def unpack_rows(idx, rec):
    n = idx.shape[0]

    def kernel(idx_ref, rec_ref, out_ref):
        def blk(b, c):
            for j in range(UNROLL):
                out_ref[b * UNROLL + j] = rec_ref[idx_ref[b * UNROLL + j]]
            return c
        lax.fori_loop(0, n // UNROLL, blk, 0)

    return pl.pallas_call(
        kernel, out_shape=jax.ShapeDtypeStruct((n,) + rec.shape[1:], rec.dtype),
        in_specs=[SMEM_SPEC, VMEM_SPEC], out_specs=VMEM_SPEC, compiler_params=local_params(), name="unpack_rows",
        cost_estimate=cost(12, 2**23),
    )(idx, rec)


def pack_rows(pos, dst, seg, grad_own, grad_pair, n_out):
    n = grad_own.shape[0]
    tail = grad_own.shape[1:]

    def kernel(pos_ref, dst_ref, seg_ref, own_ref, pair_ref, out_ref, g_ref, sem):
        first = pltpu.make_async_copy(own_ref, g_ref.at[pl.ds(0, n)], sem.at[0])
        second = pltpu.make_async_copy(pair_ref, g_ref.at[pl.ds(n, n)], sem.at[1])
        first.start()
        second.start()
        first.wait()
        second.wait()
        length = seg_ref[0]

        def blk(b, carry):
            carry = list(carry)
            for j in range(4):
                for q in range(STREAMS):
                    k = q * length + b * 4 + j
                    acc, prev = carry[q]
                    cur = dst_ref[k]
                    row = g_ref[pos_ref[k]]
                    acc = jnp.where(cur == prev, acc + row, row)
                    out_ref[cur] = acc
                    carry[q] = (acc, cur)
            return tuple(carry)
        zero = jnp.zeros(tail, jnp.float32)
        lax.fori_loop(0, length // 4, blk, tuple((zero, jnp.int32(-1)) for _ in range(STREAMS)))

    return pl.pallas_call(
        kernel, out_shape=jax.ShapeDtypeStruct((n_out,) + tail, jnp.float32),
        in_specs=[SMEM_SPEC, SMEM_SPEC, SMEM_SPEC, ANY_SPEC, ANY_SPEC], out_specs=VMEM_SPEC,
        scratch_shapes=[pltpu.VMEM((2 * n,) + tail, jnp.float32), pltpu.SemaphoreType.DMA((2,))],
        compiler_params=local_params(), name="pack_rows", cost_estimate=cost(30, 2**24),
    )(pos, dst, seg, grad_own, grad_pair)


def owner_scatter(ids, rec, rows):
    n_src = ids.shape[0] // IDW
    tail = rec.shape[1:]

    def kernel(ids_ref, rec_ref, out_ref, accs):
        def zero(i, c):
            for a in accs:
                a[pl.ds(i * 64, 64)] = jnp.zeros((64,) + tail, jnp.float32)
            return c
        lax.fori_loop(0, rows // 64, zero, 0)

        def src(s, c):
            n = ids_ref[s * IDW + IDW - 1]

            def blk(b, c):
                for j in range(ACCS):
                    r = b * ACCS + j
                    idx = jnp.where(r < n, ids_ref[s * IDW + r] & (rows - 1), rows)
                    accs[j][idx] = accs[j][idx] + rec_ref[s * SLOTS + r]
                return c
            lax.fori_loop(0, (n + ACCS - 1) // ACCS, blk, 0)
            return c
        lax.fori_loop(0, n_src, src, 0)

        def fin(i, c):
            v = accs[0][pl.ds(i * 64, 64)]
            for a in accs[1:]:
                v = v + a[pl.ds(i * 64, 64)]
            out_ref[pl.ds(i * 64, 64)] = v
            return c
        lax.fori_loop(0, rows // 64, fin, 0)

    return pl.pallas_call(
        kernel, out_shape=jax.ShapeDtypeStruct((rows,) + tail, rec.dtype),
        in_specs=[SMEM_SPEC, VMEM_SPEC], out_specs=VMEM_SPEC,
        scratch_shapes=[[pltpu.VMEM((rows + 8,) + tail, rec.dtype) for _ in range(ACCS)]],
        compiler_params=local_params(), name="owner_scatter", cost_estimate=cost(30, 2**24),
    )(ids, rec)


def greet(partners):
    barrier = pltpu.get_barrier_semaphore()
    for p in partners:
        pl.semaphore_signal(barrier, inc=1, device_id=(p,), device_id_type=MESH)
    pl.semaphore_wait(barrier, len(partners))


def chip_exchange(blocks, cid, n_chip):
    def kernel(x_ref, o_ref, ssem, rsem, lsem):
        me = lax.axis_index('emb')
        chip = me // 2
        greet([me ^ (2 * d) for d in range(1, n_chip)])
        copies = [pltpu.make_async_copy(x_ref.at[chip], o_ref.at[chip], lsem)]
        for d in range(1, n_chip):
            copies.append(pltpu.make_async_remote_copy(
                src_ref=x_ref.at[chip ^ d], dst_ref=o_ref.at[chip], send_sem=ssem.at[d], recv_sem=rsem.at[d],
                device_id=(me ^ (2 * d),), device_id_type=MESH))
        for c in copies:
            c.start()
        for c in copies:
            c.wait()

    return pl.pallas_call(
        kernel, out_shape=jax.ShapeDtypeStruct(blocks.shape, blocks.dtype), in_specs=[ANY_SPEC], out_specs=ANY_SPEC,
        scratch_shapes=[pltpu.SemaphoreType.DMA((n_chip,)), pltpu.SemaphoreType.DMA((n_chip,)), pltpu.SemaphoreType.DMA],
        compiler_params=remote_params(cid), name="chip_exchange", cost_estimate=cost(100, 2**23))(blocks)


def fetch_exchange(blocks, cid, n_chip):
    def kernel(x_ref, o_ref, ssem, rsem, fssem, frsem, lsem):
        me = lax.axis_index('emb')
        chip, core = me // 2, lax.rem(me, 2)
        greet([me ^ (2 * d) for d in range(1, n_chip)] + [me ^ 1])
        own = pltpu.make_async_copy(x_ref.at[chip], o_ref.at[core, chip], lsem)
        own.start()
        sends, passes = [], []
        for d in range(1, n_chip):
            sends.append(pltpu.make_async_remote_copy(
                src_ref=x_ref.at[chip ^ d], dst_ref=o_ref.at[core, chip], send_sem=ssem.at[d], recv_sem=rsem.at[d],
                device_id=(me ^ (2 * d),), device_id_type=MESH))
            sends[-1].start()

        def forward(src, d):
            passes.append(pltpu.make_async_remote_copy(
                src_ref=src, dst_ref=o_ref.at[core, chip ^ d], send_sem=fssem.at[d], recv_sem=frsem.at[d],
                device_id=(me ^ 1,), device_id_type=MESH))
            passes[-1].start()
        forward(x_ref.at[chip], 0)
        for d in range(1, n_chip):
            pltpu.make_async_remote_copy(
                src_ref=x_ref.at[chip ^ d], dst_ref=o_ref.at[core, chip ^ d], send_sem=ssem.at[d], recv_sem=rsem.at[d],
                device_id=(me ^ (2 * d),), device_id_type=MESH).wait_recv()
            forward(o_ref.at[core, chip ^ d], d)
        own.wait()
        for c in sends:
            c.wait_send()
        for d in range(n_chip):
            passes[d].wait_send()
            pltpu.make_async_remote_copy(
                src_ref=x_ref.at[chip ^ d], dst_ref=o_ref.at[1 - core, chip ^ d], send_sem=fssem.at[d], recv_sem=frsem.at[d],
                device_id=(me ^ 1,), device_id_type=MESH).wait_recv()

    return pl.pallas_call(
        kernel, out_shape=jax.ShapeDtypeStruct((2,) + blocks.shape, blocks.dtype), in_specs=[ANY_SPEC], out_specs=ANY_SPEC,
        scratch_shapes=[pltpu.SemaphoreType.DMA((n_chip,))] * 4 + [pltpu.SemaphoreType.DMA],
        compiler_params=remote_params(cid), name="fetch_exchange", cost_estimate=cost(60, 2**23))(blocks)


def plane_exchange(rows3, cid, to_owner):
    n_row = rows3.shape[0]
    blk = n_row // PLANE

    def kernel(x_ref, o_ref, ssem, rsem, lsem):
        me = lax.axis_index('emb')
        place = lax.rem(me, PLANE)
        greet([me ^ b for b in range(1, PLANE)])

        def rows_of(b):
            src, dst = (place ^ b, b) if to_owner else (b, place)
            return x_ref.at[pl.ds(src * blk, blk)], o_ref.at[pl.ds(dst * blk, blk)]
        copies = [pltpu.make_async_copy(*rows_of(0), lsem)]
        for b in range(1, PLANE):
            src, dst = rows_of(b)
            copies.append(pltpu.make_async_remote_copy(
                src_ref=src, dst_ref=dst, send_sem=ssem.at[b], recv_sem=rsem.at[b],
                device_id=(me ^ b,), device_id_type=MESH))
        for c in copies:
            c.start()
        for c in copies:
            c.wait()

    return pl.pallas_call(
        kernel, out_shape=jax.ShapeDtypeStruct(rows3.shape, rows3.dtype), in_specs=[ANY_SPEC], out_specs=ANY_SPEC,
        scratch_shapes=[pltpu.SemaphoreType.DMA((PLANE,)), pltpu.SemaphoreType.DMA((PLANE,)), pltpu.SemaphoreType.DMA],
        compiler_params=remote_params(cid), name="plane_exchange", cost_estimate=cost(40, 2**23))(rows3)


def route_plan(ids_pair, n_own, rows_dev, n_dev, core):
    n = ids_pair.shape[1]
    n_chip = n_dev // 2
    blk = rows_dev // PLANE
    owner, local = ids_pair // rows_dev, lax.rem(ids_pair, rows_dev)
    place = lax.rem(owner, PLANE)
    server = (owner - place) + ((local // blk) ^ place)
    name = (lax.rem(server, 2) * n_chip + server // 2) * rows_dev + place * blk + lax.rem(local, blk)
    lane = lax.broadcasted_iota(jnp.int32, ids_pair.shape, 1)
    key = lax.sort(name * n + lane, dimension=1)
    sid, pos = key // n, lax.rem(key, n)
    half = sid // (n_chip * rows_dev)
    n_low = jnp.sum((half == 0).astype(jnp.int32), axis=1, keepdims=True)
    sizes = jnp.concatenate([n_low, n - n_low], axis=1)
    segs = (sizes + 4 * STREAMS - 1) // (4 * STREAMS) * 4
    rel = lane - half * n_low
    seg = jnp.where(half == 0, segs[:, :1], segs[:, 1:])
    prev = jnp.concatenate([jnp.full_like(sid[:, :1], -1), sid[:, :-1]], axis=1)
    first = sid != prev
    for q in range(1, STREAMS):
        first = first | (rel == q * seg)
    slot = jnp.cumsum(first.astype(jnp.int32), axis=1) - 1
    tgt = sid // rows_dev
    bound = jnp.arange(n_dev + 1, dtype=jnp.int32)
    below = first[:, None, :] & (tgt[:, None, :] < bound[None, :, None])
    start = jnp.sum(below.astype(jnp.int32), axis=2)
    mine = (tgt[:, None, :] == bound[None, :-1, None])
    rank = slot - jnp.sum(jnp.where(mine, start[:, :-1, None], 0), axis=1)
    span = 2 * rows_dev
    code = tgt * span + rank
    by_pos = lax.sort(jnp.where(pos < n_own, pos * (n_dev * span) + code, jnp.iinfo(jnp.int32).max), dimension=1)
    code_own = lax.rem(by_pos[:, :n_own], n_dev * span)
    uid = lax.sort(jnp.where(first, sid, jnp.iinfo(jnp.int32).max), dimension=1)
    uid = jnp.concatenate([uid, jnp.zeros((uid.shape[0], SLOTS), jnp.int32)], axis=1)
    count = start[:, 1:] - start[:, :-1]
    size = jnp.where(core == 0, sizes[:, 0], sizes[:, 1])
    begin = jnp.where(core == 0, 0, n_low[:, 0])
    both = jnp.stack([pos, code], axis=1)
    reach = n + 4 * STREAMS
    both = jnp.concatenate([both, both, both[:, :, :4 * STREAMS]], axis=2)
    mine_list = jnp.stack([lax.dynamic_slice(both[t], (0, begin[t]), (2, reach)) for t in range(both.shape[0])])
    valid = jnp.arange(reach, dtype=jnp.int32)[None, :] < size[:, None]
    pos_half = jnp.where(valid, mine_list[:, 0], 0)
    code_half = jnp.where(valid, mine_list[:, 1], -1)
    seg_half = jnp.where(core == 0, segs[:, 0], segs[:, 1])
    return dict(pos=pos_half, code=code_half, seg=seg_half, code_own=code_own, uid=uid,
                start=lax.dynamic_slice(start, (0, core * n_chip), (start.shape[0], n_chip)),
                count=lax.dynamic_slice(count, (0, core * n_chip), (count.shape[0], n_chip)),
                peak=jnp.max(count, axis=1), span=span)


def round_slot(code, span, rnd, trash, tgt_mod):
    tgt, rank = code // span, lax.rem(code, span)
    rank = rank - rnd * SLOTS
    inside = (code >= 0) & (rank >= 0) & (rank < SLOTS)
    return jnp.where(inside, lax.rem(tgt, tgt_mod) * SLOTS + rank, trash)


def solution(mesh):
    n_dev = mesh.shape['emb']
    n_chip = n_dev // 2
    tok_spec = P('emb', None)
    tab_spec = P(None, 'emb', None)
    pairs = [(i, i ^ 1) for i in range(n_dev)]

    def local_program(x_start, d_out, token_ids, w_up, w_down, w_gate, w_proj, tables):
        n_tab, n_tok, n_heads = token_ids.shape
        rows_dev, row_width = tables.shape[1], tables.shape[2]
        n_req = n_tok * n_heads
        tail = (row_width // 128, 128)
        core = lax.rem(lax.axis_index('emb'), 2)
        layers = w_up.shape[0]
        slot_of = {1: 0, layers - 1: 1}

        flat_ids = token_ids.reshape(n_tab, n_req)
        plan = route_plan(jnp.concatenate([flat_ids, lax.ppermute(flat_ids, 'emb', pairs)], axis=1),
                          n_req, rows_dev, n_dev, core)
        served = plane_exchange(tables.reshape((n_tab, rows_dev) + tail).transpose(1, 0, 2, 3), 0, False)

        def trade_ids(rnd, cid):
            blocks = make_ids(plan['uid'], plan['start'], plan['count'], plan['peak'], rnd)
            got = chip_exchange(blocks.reshape(n_chip, n_tab * IDW // 128, 128), cid, n_chip)
            got = got.reshape(n_chip, n_tab, IDW)
            return got, [got[:, t].reshape(n_chip * IDW) for t in range(n_tab)]

        got0, ids0 = trade_ids(jnp.int32(0), 1)
        rounds = (jnp.max(got0[:, :, IDW - 2], axis=0) + SLOTS - 1) // SLOTS

        def fetch(which, ids, rnd, cid):
            sent = owner_gather(ids, served[:, which]).reshape((n_chip, SLOTS) + tail)
            rec = fetch_exchange(sent, cid, n_chip).reshape((2 * n_chip * SLOTS,) + tail)
            idx = round_slot(plan['code_own'][which], plan['span'], rnd, 0, n_dev)
            return unpack_rows(idx, rec)

        def fetch_rows(which):
            def more(state):
                rnd, rows = state
                _, ids = trade_ids(rnd, 2 + which)
                new = fetch(which, ids[which], rnd, 4 + which)
                rank = lax.rem(plan['code_own'][which], plan['span'])
                return rnd + 1, jnp.where((rank // SLOTS == rnd)[:, None, None], new, rows)
            first = fetch(which, ids0[which], 0, 6 + which)
            _, rows = lax.while_loop(lambda s: s[0] < rounds[which], more, (jnp.int32(1), first))
            return rows.reshape(n_tok, n_heads * row_width)

        def give(which, grad_own, grad_pair, ids, rnd, cid):
            n_slot = n_chip * SLOTS
            dst = round_slot(plan['code'][which], plan['span'], rnd, n_slot, n_chip)
            sent = pack_rows(plan['pos'][which], dst, plan['seg'][which:which + 1], grad_own, grad_pair, n_slot + 8)
            rec = chip_exchange(sent[:n_slot].reshape((n_chip, SLOTS) + tail), cid, n_chip)
            return owner_scatter(ids, rec.reshape((n_slot,) + tail), rows_dev)

        def return_rows(which, grad_rows):
            grad_own = grad_rows.reshape((n_req,) + tail)
            grad_pair = lax.ppermute(grad_own, 'emb', pairs)

            def more(state):
                rnd, total = state
                _, ids = trade_ids(rnd, 8 + which)
                return rnd + 1, total + give(which, grad_own, grad_pair, ids[which], rnd, 10 + which)
            first = give(which, grad_own, grad_pair, ids0[which], 0, 12 + which)
            _, total = lax.while_loop(lambda s: s[0] < rounds[which], more, (jnp.int32(1), first))
            return plane_exchange(total, 14 + which, True).reshape(rows_dev, row_width)

        emb = [fetch_rows(which) for which in range(n_tab)]
        saved_acts = []
        x_cur = x_start
        for layer_idx in range(layers):
            normed, inv_rms = norm_fwd(x_cur)
            hidden = jnp.dot(normed, w_up[layer_idx], preferred_element_type=jnp.float32).astype(jnp.bfloat16)
            activated = gelu_fn(hidden.astype(jnp.float32)).astype(jnp.bfloat16)
            mlp_out = jnp.dot(activated, w_down[layer_idx], preferred_element_type=jnp.float32).astype(jnp.bfloat16)
            new_res = x_cur.astype(jnp.float32) + mlp_out.astype(jnp.float32)
            gate_saved = None
            if layer_idx in slot_of:
                which = slot_of[layer_idx]
                emb_rows = emb[which]
                pre_gate = jnp.dot(normed, w_gate[which], preferred_element_type=jnp.float32).astype(jnp.bfloat16)
                gate_val = gelu_fn(pre_gate.astype(jnp.float32)).astype(jnp.bfloat16)
                mixed_val = (gate_val.astype(jnp.float32) * emb_rows.astype(jnp.float32)).astype(jnp.bfloat16)
                proj_out = jnp.dot(mixed_val, w_proj[which], preferred_element_type=jnp.float32).astype(jnp.bfloat16)
                new_res = new_res + proj_out.astype(jnp.float32)
                gate_saved = (pre_gate, gate_val, emb_rows)
            saved_acts.append((x_cur, inv_rms, hidden, gate_saved))
            x_cur = new_res.astype(jnp.bfloat16)

        grads = [None] * n_tab
        d_res = d_out.astype(jnp.float32)
        for layer_idx in reversed(range(1, layers)):
            x_prev, inv_rms, hidden, gate_saved = saved_acts[layer_idx]
            d_low = d_res.astype(jnp.bfloat16)
            if gate_saved is not None:
                which = slot_of[layer_idx]
                pre_gate, gate_val, emb_rows = gate_saved
                d_mix = jnp.einsum('td,ed->te', d_low, w_proj[which], preferred_element_type=jnp.float32)
                grads[which] = return_rows(which, gate_val.astype(jnp.float32) * d_mix)
            if layer_idx > 1:
                d_act = jnp.einsum('td,fd->tf', d_low, w_down[layer_idx], preferred_element_type=jnp.float32)
                d_hid = gelu_grad(hidden, d_act)
                d_norm = jnp.einsum('tf,df->td', d_hid.astype(jnp.bfloat16), w_up[layer_idx], preferred_element_type=jnp.float32)
                if gate_saved is not None:
                    d_gate = gelu_grad(pre_gate, d_mix * emb_rows.astype(jnp.float32))
                    d_norm = d_norm + jnp.einsum('te,de->td', d_gate.astype(jnp.bfloat16), w_gate[which], preferred_element_type=jnp.float32)
                d_res = d_res + norm_bwd(x_prev, inv_rms, d_norm)
        return x_cur, jnp.stack(grads)

    return jax.shard_map(local_program, mesh=mesh, in_specs=(tok_spec, tok_spec, tab_spec, P(), P(), P(), P(), tab_spec),
                         out_specs=(tok_spec, tab_spec), check_vma=False)
```

```python
import jax
import jax.numpy as jnp
from jax import lax
from jax.experimental import pallas as pl
from jax.experimental.pallas import tpu as pltpu
from jax.sharding import PartitionSpec as P


EPS = 1e-6
C1 = 0.7978845608028654
C2 = C1 * 0.044715
BF16 = jnp.bfloat16
F32 = jnp.float32
VMEM_LIMIT = 62 * 1024 * 1024
MESH = pl.DeviceIdType.MESH
PLANE = 8
SLOTS = 336
IDW = 1024
UNROLL = 16

SMEM_SPEC = pl.BlockSpec(memory_space=pltpu.SMEM)
VMEM_SPEC = pl.BlockSpec(memory_space=pltpu.VMEM)
ANY_SPEC = pl.BlockSpec(memory_space=pl.ANY)


def local_params():
    return pltpu.CompilerParams(vmem_limit_bytes=VMEM_LIMIT)


def remote_params(cid):
    return pltpu.CompilerParams(vmem_limit_bytes=VMEM_LIMIT, collective_id=cid, has_side_effects=True)


def cost(us, nbytes):
    return pl.CostEstimate(flops=int(us * 9 * 10**8), bytes_accessed=nbytes, transcendentals=0)


def shape_of(shape, dtype):
    return jax.ShapeDtypeStruct(shape, dtype)


def gelu(x):
    half = 0.5 * x
    return half + half * jnp.tanh(x * (C1 + C2 * (x * x)))


def gelu_bwd(x, ct):
    x2 = x * x
    t = jnp.tanh(x * (C1 + C2 * x2))
    return ct * ((0.5 + 0.5 * t) + (x * (0.5 - (0.5 * t) * t)) * (C1 + (3 * C2) * x2))


def dot_nn(a, b):
    return jnp.dot(a, b, preferred_element_type=F32)


def dot_nt(a, b):
    return lax.dot_general(a, b, (((1,), (1,)), ((), ())), preferred_element_type=F32)


def rms(x_f):
    return lax.rsqrt(jnp.mean(x_f * x_f, axis=-1, keepdims=True) + EPS)


def token_kernel(body, tile, tokens, ins, weights, outs, scratch, us):
    n_in, n_w, n_out = len(ins), len(weights), len(outs)

    def kernel(*refs):
        in_refs = refs[:n_in]
        w_hbm = refs[n_in:n_in + n_w]
        out_refs = refs[n_in + n_w:n_in + n_w + n_out]
        w_vmem = refs[n_in + n_w + n_out:n_in + 2 * n_w + n_out]
        sem = refs[n_in + 2 * n_w + n_out]
        rest = refs[n_in + 2 * n_w + n_out + 1:]
        copies = [pltpu.make_async_copy(w_hbm[i].at[weights[i][1]], w_vmem[i], sem.at[i]) for i in range(n_w)]
        opening = pl.program_id(0) == 0

        @pl.when(opening)
        def _():
            for c in copies:
                c.start()

        def need(*which):
            @pl.when(opening)
            def _():
                for i in which:
                    copies[i].wait()

        body(need, in_refs, w_vmem, out_refs, rest)

    def tiled(shape, per):
        return pl.BlockSpec((tile * per,) + shape[1:], lambda i: (i,) + (0,) * (len(shape) - 1))

    in_specs = [tiled(a.shape, per) for a, per in ins] + [ANY_SPEC] * n_w
    out_specs = [tiled(s.shape, per) for s, per in outs]
    w_scratch = [pltpu.VMEM(w.shape[1:], w.dtype) for w, _ in weights]
    return pl.pallas_call(
        kernel, grid=(tokens // tile,), out_shape=[s for s, _ in outs], in_specs=in_specs, out_specs=out_specs,
        scratch_shapes=w_scratch + [pltpu.SemaphoreType.DMA((n_w,))] + scratch,
        compiler_params=local_params(), cost_estimate=cost(us, 2**25),
    )(*[a for a, _ in ins], *[w for w, _ in weights])


def mlp_up(u, w_up, act, h_ref, chunk=512):
    for j in range(w_up.shape[1] // chunk):
        cols = slice(j * chunk, (j + 1) * chunk)
        h = dot_nn(u, w_up[:, cols]).astype(BF16)
        if h_ref is not None:
            h_ref[:, cols] = h
        if act is not None:
            act[:, cols] = gelu(h.astype(F32)).astype(BF16)


def store_rows(ref, value):
    tokens, width = value.shape
    n = width // 128
    for c in range(n):
        ref[pl.ds(c, tokens, stride=n), :] = value[:, c * 128:(c + 1) * 128]


def layer_plain(x, w_up, w_down, layer, tile=512):
    tokens, d = x.shape

    def body(need, ins, w, outs, rest):
        need(0, 1)
        x_f = ins[0][...].astype(F32)
        u = (x_f * rms(x_f)).astype(BF16)
        mlp_up(u, w[0], rest[0], None)
        for q in range(d // 256):
            cols = slice(q * 256, (q + 1) * 256)
            m = dot_nn(rest[0][...], w[1][:, cols]).astype(BF16)
            outs[0][:, cols] = (ins[0][:, cols].astype(F32) + m.astype(F32)).astype(BF16)

    return token_kernel(body, tile, tokens, [(x, 1)], [(w_up, layer), (w_down, layer)],
                        [(shape_of(x.shape, BF16), 1)], [pltpu.VMEM((tile, w_up.shape[2]), BF16)], 44)[0]


def layer_table_head(x, w_up, w_down, w_gate, layer, which, tile=512):
    tokens, d = x.shape

    def body(need, ins, w, outs, rest):
        need(0, 1, 2)
        x_f = ins[0][...].astype(F32)
        u = (x_f * rms(x_f)).astype(BF16)
        mlp_up(u, w[0], rest[0], None)
        a = dot_nn(u, w[2][...]).astype(BF16)
        outs[1][...] = gelu(a.astype(F32)).astype(BF16)
        for q in range(d // 256):
            cols = slice(q * 256, (q + 1) * 256)
            outs[0][:, cols] = dot_nn(rest[0][...], w[1][:, cols]).astype(BF16)

    return token_kernel(body, tile, tokens, [(x, 1)],
                        [(w_up, layer), (w_down, layer), (w_gate, which)],
                        [(shape_of(x.shape, BF16), 1), (shape_of(x.shape, BF16), 1)],
                        [pltpu.VMEM((tile, w_up.shape[2]), BF16)], 50)


def layer_middle(x, m, g, e, d_out, w_up, w_down, w_gate, w_proj, layer, tile=256):
    tokens, d = x.shape
    ff = w_up.shape[2]

    def body(need, ins, w, outs, rest):
        x_ref, m_ref, g_ref, e_ref, c_ref = ins
        x2_ref, h_ref, x3_ref, a_ref, dz_ref, row_ref = outs
        act = rest[0]
        need(4, 0)
        z = (g_ref[...].astype(F32) * e_ref[...].astype(F32)).astype(BF16)
        q = dot_nn(z, w[4][...]).astype(BF16)
        x2 = ((x_ref[...].astype(F32) + m_ref[...].astype(F32)) + q.astype(F32)).astype(BF16)
        x2_ref[...] = x2
        x_f = x2.astype(F32)
        u = (x_f * rms(x_f)).astype(BF16)
        need(1)
        mlp_up(u, w[0], act, h_ref)
        for n in range(d // 256):
            cols = slice(n * 256, (n + 1) * 256)
            mm = dot_nn(act[...], w[1][:, cols]).astype(BF16)
            x3_ref[:, cols] = (x2_ref[:, cols].astype(F32) + mm.astype(F32)).astype(BF16)
        x_f = x3_ref[...].astype(F32)
        u = (x_f * rms(x_f)).astype(BF16)
        need(2, 3)
        a = dot_nn(u, w[2][...]).astype(BF16)
        a_ref[...] = a
        gate = gelu(a.astype(F32)).astype(BF16)
        dz = dot_nt(c_ref[...], w[3][...])
        dz_ref[...] = dz
        store_rows(row_ref, gate.astype(F32) * dz)

    vec = (shape_of((tokens, d), BF16), 1)
    return token_kernel(body, tile, tokens, [(x, 1), (m, 1), (g, 1), (e, 1), (d_out, 1)],
                        [(w_up, layer), (w_down, layer), (w_gate, 1), (w_proj, 1), (w_proj, 0)],
                        [vec, (shape_of((tokens, ff), BF16), 1), vec, vec, (shape_of((tokens, d), F32), 1),
                         (shape_of((tokens * d // 128, 128), F32), d // 128)],
                        [pltpu.VMEM((tile, ff), BF16)], 62)


def last_up(x, w_up, layer, tile=512):
    tokens, ff = x.shape[0], w_up.shape[2]

    def body(need, ins, w, outs, rest):
        need(0)
        x_f = ins[0][...].astype(F32)
        u = (x_f * rms(x_f)).astype(BF16)
        mlp_up(u, w[0], None, outs[0])

    return token_kernel(body, tile, tokens, [(x, 1)], [(w_up, layer)],
                        [(shape_of((tokens, ff), BF16), 1)], [], 22)[0]


def last_down(x, h, a, e, w_down, w_proj, layer, which, tile=256):
    tokens, d = x.shape
    ff = h.shape[1]

    def body(need, ins, w, outs, rest):
        x_ref, h_ref, a_ref, e_ref = ins
        act = rest[0]
        need(0, 1)
        gate = gelu(a_ref[...].astype(F32)).astype(BF16)
        z = (gate.astype(F32) * e_ref[...].astype(F32)).astype(BF16)
        for j in range(ff // 512):
            cols = slice(j * 512, (j + 1) * 512)
            act[:, cols] = gelu(h_ref[:, cols].astype(F32)).astype(BF16)
        for n in range(d // 256):
            cols = slice(n * 256, (n + 1) * 256)
            m = dot_nn(act[...], w[0][:, cols]).astype(BF16)
            q = dot_nn(z, w[1][:, cols]).astype(BF16)
            outs[0][:, cols] = ((x_ref[:, cols].astype(F32) + m.astype(F32)) + q.astype(F32)).astype(BF16)

    return token_kernel(body, tile, tokens, [(x, 1), (h, 1), (a, 1), (e, 1)],
                        [(w_down, layer), (w_proj, which)], [(shape_of(x.shape, BF16), 1)],
                        [pltpu.VMEM((tile, ff), BF16)], 30)[0]


def back_mlp(c_b, h_ref, w_up, w_down, dh):
    chunk = 512
    for j in range(h_ref.shape[1] // chunk):
        cols = slice(j * chunk, (j + 1) * chunk)
        d_act = dot_nt(c_b, w_down[cols, :])
        dh[:, cols] = gelu_bwd(h_ref[:, cols].astype(F32), d_act).astype(BF16)
    return jnp.concatenate([dot_nt(dh[...], w_up[n * 256:(n + 1) * 256, :]) for n in range(w_up.shape[0] // 256)], axis=1)


def back_norm(c_f, x_ref, du):
    x_f = x_ref[...].astype(F32)
    s = rms(x_f)
    return c_f + (s * du - x_f * (s * s * s) * jnp.mean(x_f * du, axis=-1, keepdims=True))


def back_table(c, h, x, a, dz, e, w_up, w_down, w_gate, layer, which, tile=256):
    tokens, d = x.shape
    ff = h.shape[1]

    def body(need, ins, w, outs, rest):
        c_ref, h_ref, x_ref, a_ref, dz_ref, e_ref = ins
        need(0, 1, 2)
        d_gate = gelu_bwd(a_ref[...].astype(F32), dz_ref[...] * e_ref[...].astype(F32)).astype(BF16)
        rest[1][...] = dot_nt(d_gate, w[2][...])
        du = back_mlp(c_ref[...], h_ref, w[0], w[1], rest[0]) + rest[1][...]
        outs[0][...] = back_norm(c_ref[...].astype(F32), x_ref, du)

    return token_kernel(body, tile, tokens,
                        [(c, 1), (h, 1), (x, 1), (a, 1), (dz, 1), (e, 1)],
                        [(w_up, layer), (w_down, layer), (w_gate, which)],
                        [(shape_of((tokens, d), F32), 1)],
                        [pltpu.VMEM((tile, ff), BF16), pltpu.VMEM((tile, d), F32)], 58)[0]


def back_plain(c, h, x, g, w_up, w_down, w_proj, layer, which, tile=256):
    tokens, d = x.shape
    ff = h.shape[1]

    def body(need, ins, w, outs, rest):
        c_ref, h_ref, x_ref, g_ref = ins
        need(0, 1, 2)
        du = back_mlp(c_ref[...].astype(BF16), h_ref, w[0], w[1], rest[0])
        c_low = back_norm(c_ref[...], x_ref, du).astype(BF16)
        store_rows(outs[0], g_ref[...].astype(F32) * dot_nt(c_low, w[2][...]))

    return token_kernel(body, tile, tokens, [(c, 1), (h, 1), (x, 1), (g, 1)],
                        [(w_up, layer), (w_down, layer), (w_proj, which)],
                        [(shape_of((tokens * d // 128, 128), F32), d // 128)],
                        [pltpu.VMEM((tile, ff), BF16)], 58)[0]


def split_rows(tables, place):
    n_tab, rows, width = tables.shape
    blk = rows // PLANE

    def kernel(place_ref, src, out, buf, isem, osem):
        reads = [pltpu.make_async_copy(src.at[t], buf.at[t], isem.at[t]) for t in range(n_tab)]
        for c in reads:
            c.start()
        writes = []
        for t in range(n_tab):
            reads[t].wait()
            for b in range(PLANE):
                writes.append(pltpu.make_async_copy(buf.at[t, pl.ds(b * blk, blk)], out.at[place_ref[0] ^ b, t], osem.at[t * PLANE + b]))
                writes[-1].start()
        for c in writes:
            c.wait()

    return pl.pallas_call(
        kernel, out_shape=shape_of((PLANE, n_tab, blk, width), tables.dtype), in_specs=[SMEM_SPEC, ANY_SPEC], out_specs=ANY_SPEC,
        scratch_shapes=[pltpu.VMEM(tables.shape, tables.dtype), pltpu.SemaphoreType.DMA((n_tab,)),
                        pltpu.SemaphoreType.DMA((n_tab * PLANE,))],
        compiler_params=local_params(), name="split_rows", cost_estimate=cost(4, 2**23))(place, tables)


def make_ids(uid, start, count, peak, rnd, blank):
    n_tgt = count.shape[0]
    rows = -(-SLOTS // 128)

    def kernel(uid_ref, start_ref, count_ref, peak_ref, rnd_ref, out_ref):
        lane = lax.broadcasted_iota(jnp.int32, (1, 128), 1)
        out_ref[...] = jnp.full(out_ref.shape, peak_ref[0], jnp.int32)
        for g in range(n_tgt):
            shift = rnd_ref[0] * SLOTS
            left = jnp.clip(count_ref[g] - shift, 0, SLOTS)
            at = jnp.minimum(start_ref[g] + shift, (uid_ref.shape[0] - rows - 1) * 128)
            row, off = at // 128, lax.rem(at, 128)
            turned = [pltpu.roll(uid_ref[row + i], lax.rem(128 - off, 128), axis=1) for i in range(rows + 1)]
            for i in range(rows):
                ids = jnp.where(lane < 128 - off, turned[i], turned[i + 1])
                out_ref[g, i:i + 1, :] = jnp.where(i * 128 + lane < left, ids, blank)

    return pl.pallas_call(
        kernel, out_shape=shape_of((n_tgt, IDW // 128, 128), jnp.int32),
        in_specs=[VMEM_SPEC] + [SMEM_SPEC] * 4, out_specs=VMEM_SPEC, compiler_params=local_params(), name="make_ids",
        cost_estimate=cost(3, 2**18),
    )(uid, start, count, peak, jnp.reshape(rnd, (1,)).astype(jnp.int32))


def pair_at(index):
    return pl.ds(pl.multiple_of(index, 2), 2)


def owner_gather(ids, served, which, n_src):
    blk, width = served.shape[2:]
    rows = PLANE * blk
    pieces = width // 128

    def kernel(ids_ref, served_ref, out_ref, native, flat, isem):
        reads = [pltpu.make_async_copy(served_ref.at[b, which], native.at[b], isem.at[b]) for b in range(PLANE)]
        for c in reads:
            c.start()
        for b in range(PLANE):
            reads[b].wait()
            for c in range(pieces):
                flat[pl.ds(b * blk * pieces + c, blk, stride=pieces), :] = native[b, :, c * 128:(c + 1) * 128].astype(F32)

        def src(s, c):
            def part(b, c):
                for j in range(UNROLL):
                    r = b * UNROLL + j
                    out_ref[s * SLOTS + r] = flat[pair_at(ids_ref[s * IDW + r]), :].astype(BF16)
                return c

            lax.fori_loop(0, SLOTS // UNROLL, part, 0)
            return c

        lax.fori_loop(0, n_src, src, 0)

    return pl.pallas_call(
        kernel, out_shape=shape_of((n_src * SLOTS, pieces, 128), BF16),
        in_specs=[SMEM_SPEC, ANY_SPEC], out_specs=VMEM_SPEC,
        scratch_shapes=[pltpu.VMEM((PLANE, blk, width), BF16), pltpu.VMEM((rows * pieces + 8, 128), F32),
                        pltpu.SemaphoreType.DMA((PLANE,))],
        compiler_params=local_params(), name="owner_gather", cost_estimate=cost(14, 2**22),
    )(ids, served)


def unpack_rows(idx, rec_own, rec_pair, heads):
    n = idx.shape[0]
    half, pieces = rec_own.shape[0], rec_own.shape[1]
    tokens, tile = n // heads, 256
    per = heads * pieces

    def kernel(idx_ref, own_ref, pair_ref, out_ref, rec, stage, sem):
        copies = [pltpu.make_async_copy(own_ref, rec.at[pl.ds(0, half)], sem.at[0]),
                  pltpu.make_async_copy(pair_ref, rec.at[pl.ds(half, half)], sem.at[1])]
        for c in copies:
            c.start()
        for c in copies:
            c.wait()

        def part(i, c):
            def blk(b, c):
                for j in range(UNROLL):
                    row = rec[idx_ref[i * (tile * heads) + b * UNROLL + j]]
                    stage[pl.ds(pl.multiple_of(b * UNROLL * pieces, UNROLL * pieces) + pieces * j, pieces), :] = row.astype(F32)
                return c

            lax.fori_loop(0, tile * heads // UNROLL, blk, 0)
            for c in range(per):
                out_ref[pl.ds(i * tile, tile), c * 128:(c + 1) * 128] = stage[pl.ds(c, tile, stride=per), :].astype(BF16)
            return c

        lax.fori_loop(0, tokens // tile, part, 0)

    return pl.pallas_call(
        kernel, out_shape=shape_of((tokens, per * 128), BF16),
        in_specs=[SMEM_SPEC, ANY_SPEC, ANY_SPEC], out_specs=VMEM_SPEC,
        scratch_shapes=[pltpu.VMEM((2 * half, pieces, 128), BF16), pltpu.VMEM((tile * per, 128), F32), pltpu.SemaphoreType.DMA((2,))],
        compiler_params=local_params(), name="unpack_rows", cost_estimate=cost(16, 2**23),
    )(idx, rec_own, rec_pair)


def pack_rows(pos, dst, size, grad_own, grad_pair, n_tgt):
    n = grad_own.shape[0]
    n_row = 2 * n_tgt * SLOTS
    low = jnp.iinfo(jnp.int32).max

    def kernel(pos_ref, dst_ref, size_ref, own_ref, pair_ref, out_ref, g_ref, stage, sem):
        first = pltpu.make_async_copy(own_ref, g_ref.at[pl.ds(0, n)], sem.at[0])
        second = pltpu.make_async_copy(pair_ref, g_ref.at[pl.ds(n, n)], sem.at[1])
        first.start()
        second.start()
        first.wait()
        second.wait()

        def blk(b, acc):
            for j in range(UNROLL):
                p = pos_ref[b * UNROLL + j]
                row = g_ref[pair_at(p & low), :]
                acc = row + jnp.where(jnp.full((2, 128), p, jnp.int32) < 0, acc, 0.0)
                stage[pair_at(dst_ref[b * UNROLL + j]), :] = acc
            return acc

        lax.fori_loop(0, (size_ref[0] + UNROLL - 1) // UNROLL, blk, jnp.zeros((2, 128), F32))
        done = pltpu.make_async_copy(stage.at[pl.ds(0, n_row)], out_ref, sem.at[0])
        done.start()
        done.wait()

    return pl.pallas_call(
        kernel, out_shape=shape_of((n_row, 128), F32),
        in_specs=[SMEM_SPEC, SMEM_SPEC, SMEM_SPEC, ANY_SPEC, ANY_SPEC], out_specs=ANY_SPEC,
        scratch_shapes=[pltpu.VMEM((2 * n, 128), F32), pltpu.VMEM((n_row + 8, 128), F32), pltpu.SemaphoreType.DMA((2,))],
        compiler_params=local_params(), name="pack_rows", cost_estimate=cost(26, 2**24),
    )(pos, dst, size, grad_own, grad_pair)


def owner_scatter(ids, rec, rows, place):
    n_src = rec.shape[0] // (2 * SLOTS)
    per = UNROLL

    blk_rows = 2 * rows // PLANE

    def kernel(ids_ref, place_ref, rec_ref, *refs):
        outs, (acc, buf, sem, osem) = refs[:PLANE], refs[PLANE:]
        reads = [pltpu.make_async_copy(rec_ref.at[pl.ds(s * 2 * SLOTS, 2 * SLOTS)], buf.at[pl.ds(s * 2 * SLOTS, 2 * SLOTS)], sem.at[s])
                 for s in range(n_src)]
        for c in reads:
            c.start()

        def zero(i, c):
            acc[pl.ds(i * 128, 128), :] = jnp.zeros((128, 128), F32)
            return c

        lax.fori_loop(0, 2 * rows // 128, zero, 0)
        for c in reads:
            c.wait()

        def src(s, c):
            def blk(b, c):
                at = [pair_at(ids_ref[s * IDW + b * per + j]) for j in range(per)]
                base = pl.multiple_of((s * SLOTS + b * per) * 2, 2 * per)
                new = [acc[i, :] + buf[pl.ds(base + 2 * j, 2), :] for j, i in enumerate(at)]
                for i, v in zip(at, new):
                    acc[i, :] = v
                return c

            lax.fori_loop(0, SLOTS // per, blk, 0)
            return c

        lax.fori_loop(0, n_src, src, 0)
        writes = []
        for b in range(PLANE):
            at = pl.multiple_of((place_ref[0] ^ b) * blk_rows, blk_rows)
            writes.append(pltpu.make_async_copy(acc.at[pl.ds(at, blk_rows)], outs[b], osem.at[b]))
            writes[-1].start()
        for c in writes:
            c.wait()

    return pl.pallas_call(
        kernel, out_shape=[shape_of((blk_rows, 128), F32)] * PLANE, in_specs=[SMEM_SPEC, SMEM_SPEC, ANY_SPEC],
        out_specs=[ANY_SPEC] * PLANE,
        scratch_shapes=[pltpu.VMEM((2 * rows + 8, 128), F32), pltpu.VMEM((n_src * 2 * SLOTS, 128), F32),
                        pltpu.SemaphoreType.DMA((n_src,)), pltpu.SemaphoreType.DMA((PLANE,))],
        compiler_params=local_params(), name="owner_scatter", cost_estimate=cost(20, 2**24),
    )(ids, place, rec)


def finish_table(blocks, grads, which, n_tab):
    blk_rows = blocks[0].shape[0]
    blk = blk_rows // 2
    shape = (n_tab, PLANE * blk, 256)
    first = grads is None

    def kernel(*refs):
        out, buf, stage, isem, osem = refs[-5:]
        reads = [pltpu.make_async_copy(refs[b], buf.at[b], isem.at[b]) for b in range(PLANE)]
        for c in reads:
            c.start()
        writes = []
        for b in range(PLANE):
            reads[b].wait()
            for c in range(2):
                stage[b, :, c * 128:(c + 1) * 128] = buf[b, pl.ds(c, blk, stride=2), :]
            writes.append(pltpu.make_async_copy(stage.at[b], out.at[which, pl.ds(b * blk, blk)], osem.at[b]))
            writes[-1].start()
        for c in writes:
            c.wait()

    args = list(blocks) + ([] if first else [grads])
    return pl.pallas_call(
        kernel, out_shape=shape_of(shape, F32), in_specs=[ANY_SPEC] * len(args), out_specs=ANY_SPEC,
        scratch_shapes=[pltpu.VMEM((PLANE, blk_rows, 128), F32), pltpu.VMEM((PLANE, blk, 256), F32),
                        pltpu.SemaphoreType.DMA((PLANE,)), pltpu.SemaphoreType.DMA((PLANE,))],
        input_output_aliases={} if first else {PLANE: 0},
        compiler_params=local_params(), name="finish_table", cost_estimate=cost(8, 2**23))(*args)


def swap_cores(x, n_dev):
    return lax.ppermute(x, 'emb', [(i, i ^ 1) for i in range(n_dev)])


def chip_trade(x, n_dev):
    groups = [list(range(c, n_dev, 2)) for c in range(2)]
    return lax.all_to_all(x, 'emb', 0, 0, axis_index_groups=groups, tiled=True)


def chip_exchange(blocks, cid, n_chip):
    def kernel(x_ref, o_ref, ssem, rsem, lsem):
        me = lax.axis_index('emb')
        chip = me // 2
        barrier = pltpu.get_barrier_semaphore()
        for d in range(1, n_chip):
            pl.semaphore_signal(barrier, inc=1, device_id=(me ^ (2 * d),), device_id_type=MESH)
        pl.semaphore_wait(barrier, n_chip - 1)
        copies = [pltpu.make_async_copy(x_ref.at[chip], o_ref.at[chip], lsem)]
        for d in range(1, n_chip):
            copies.append(pltpu.make_async_remote_copy(
                src_ref=x_ref.at[chip ^ d], dst_ref=o_ref.at[chip], send_sem=ssem.at[d], recv_sem=rsem.at[d],
                device_id=(me ^ (2 * d),), device_id_type=MESH))
        for c in copies:
            c.start()
        for c in copies:
            c.wait()

    return pl.pallas_call(
        kernel, out_shape=shape_of(blocks.shape, blocks.dtype), in_specs=[ANY_SPEC], out_specs=ANY_SPEC,
        scratch_shapes=[pltpu.SemaphoreType.DMA((n_chip,)), pltpu.SemaphoreType.DMA((n_chip,)), pltpu.SemaphoreType.DMA],
        compiler_params=remote_params(cid), name="chip_exchange", cost_estimate=cost(100, 2**23))(blocks)


def plane_trade(x, n_dev):
    groups = [list(range(z, z + PLANE)) for z in range(0, n_dev, PLANE)]
    return lax.all_to_all(x, 'emb', 0, 0, axis_index_groups=groups, tiled=True)


def place_trade(blocks, n_dev):
    return [blocks[0]] + [lax.ppermute(blocks[b], 'emb', [(i, i ^ b) for i in range(n_dev)]) for b in range(1, PLANE)]


def place_exchange(blocks, cid):
    def kernel(*refs):
        srcs, outs, (ssem, rsem) = refs[:PLANE - 1], refs[PLANE - 1:2 * (PLANE - 1)], refs[-2:]
        me = lax.axis_index('emb')
        barrier = pltpu.get_barrier_semaphore()
        for b in range(1, PLANE):
            pl.semaphore_signal(barrier, inc=1, device_id=(me ^ b,), device_id_type=MESH)
        pl.semaphore_wait(barrier, PLANE - 1)
        copies = [pltpu.make_async_remote_copy(
            src_ref=srcs[b - 1], dst_ref=outs[b - 1], send_sem=ssem.at[b], recv_sem=rsem.at[b],
            device_id=(me ^ b,), device_id_type=MESH) for b in range(1, PLANE)]
        for c in copies:
            c.start()
        for c in copies:
            c.wait()

    shape = shape_of(blocks[0].shape, blocks[0].dtype)
    got = pl.pallas_call(
        kernel, out_shape=[shape] * (PLANE - 1), in_specs=[ANY_SPEC] * (PLANE - 1), out_specs=[ANY_SPEC] * (PLANE - 1),
        scratch_shapes=[pltpu.SemaphoreType.DMA((PLANE,)), pltpu.SemaphoreType.DMA((PLANE,))],
        compiler_params=remote_params(cid), name="place_exchange", cost_estimate=cost(50, 2**22))(*blocks[1:])
    return [blocks[0]] + list(got)


def after(x, *deps):
    return lax.optimization_barrier((x,) + deps)[0]


def route_plan(ids_pair, n_own, rows_dev, n_dev, me):
    n = ids_pair.shape[0]
    n_chip = n_dev // 2
    blk = rows_dev // PLANE
    owner, local = ids_pair // rows_dev, lax.rem(ids_pair, rows_dev)
    server = owner ^ (local // blk)
    name = (lax.rem(server, 2) * n_chip + server // 2) * rows_dev + lax.rem(owner, PLANE) * blk + lax.rem(local, blk)
    lane = jnp.arange(n, dtype=jnp.int32)
    key = lax.sort(name * n + lane)
    sid, pos = key // n, lax.rem(key, n)
    n_low = jnp.sum((sid < n_chip * rows_dev).astype(jnp.int32))
    first = sid != jnp.concatenate([jnp.full((1,), -1, jnp.int32), sid[:-1]])
    slot = jnp.cumsum(first.astype(jnp.int32)) - 1
    tgt = sid // rows_dev
    bound = jnp.arange(n_dev + 1, dtype=jnp.int32)
    start = jnp.sum((first[None, :] & (tgt[None, :] < bound[:, None])).astype(jnp.int32), axis=1)
    rank = slot - jnp.sum(jnp.where(tgt[None, :] == bound[:-1, None], start[:-1, None], 0), axis=0)
    code = tgt * (2 * rows_dev) + rank
    count = start[1:] - start[:-1]
    core = lax.rem(me, 2)
    size = jnp.where(core == 0, n_low, n - n_low)
    begin = jnp.where(core == 0, 0, n_low)
    low = jnp.iinfo(jnp.int32).min
    both = jnp.stack([2 * pos + jnp.where(first, 0, low), code])
    both = jnp.concatenate([both, both, both[:, :UNROLL]], axis=1)
    mine = lax.dynamic_slice(both, (0, begin), (2, n + UNROLL))
    valid = jnp.arange(n + UNROLL, dtype=jnp.int32) < size
    most = jnp.iinfo(jnp.int32).max
    uid = lax.sort(jnp.where(first & (sid // (n_chip * rows_dev) == core), sid, most))
    uid = jnp.concatenate([2 * lax.rem(uid, rows_dev), jnp.zeros((512,), jnp.int32)]).reshape((n + 512) // 128, 1, 128)
    start = lax.dynamic_slice(start, (core * n_chip,), (n_chip,))
    return dict(pos=jnp.where(valid, mine[0], 0), code=jnp.where(valid, mine[1], -1), uid=uid, start=start - start[0],
                size=size.reshape(1), by_pos=jnp.where(pos < n_own, pos * (n_dev * 2 * rows_dev) + code, most),
                count=lax.dynamic_slice(count, (core * n_chip,), (n_chip,)), peak=jnp.max(count).reshape(1))


def round_slot(code, span, rnd, trash, width):
    tgt, rank = code // span, lax.rem(code, span) - rnd * SLOTS
    inside = (code >= 0) & (rank >= 0) & (rank < SLOTS)
    return jnp.where(inside, tgt * width + rank, trash)


def solution(mesh):
    n_dev = mesh.shape['emb']
    n_chip = n_dev // 2
    tok_spec = P('emb', None)
    tab_spec = P(None, 'emb', None)

    def step(x_start, d_out, token_ids, w_up, w_down, w_gate, w_proj, tables):
        n_tab, n_tok, n_heads = token_ids.shape
        rows_dev, row_width = tables.shape[1], tables.shape[2]
        n_req = n_tok * n_heads
        tail = (row_width // 128, 128)
        me = lax.axis_index('emb')
        core = lax.rem(me, 2)

        flat_ids = token_ids.reshape(n_tab, n_req)
        ids_pair = jnp.concatenate([flat_ids, swap_cores(flat_ids, n_dev)], axis=1)
        place = lax.rem(me, PLANE).reshape(1)
        split = split_rows(tables, place)
        served = plane_trade(split, n_dev)
        plans = [route_plan(after(ids_pair, split)[t], n_req, rows_dev, n_dev, me) for t in range(n_tab)]

        span = 2 * rows_dev
        in_order = lax.sort(jnp.stack([plan['by_pos'] for plan in plans]), dimension=1)
        code_own = lax.rem(in_order[:, :n_req], n_dev * span)

        def half_slot(plan, rnd, width, trash):
            code = plan['code']
            code = jnp.where(code >= 0, lax.rem(code, n_chip * span), code)
            return round_slot(code, span, rnd, trash, width)

        def id_blocks(which, rnd):
            plan = plans[which]
            return make_ids(plan['uid'], plan['start'], plan['count'], plan['peak'], rnd, 2 * rows_dev)

        blocks = jnp.stack([id_blocks(t, jnp.int32(0)) for t in range(n_tab)], axis=1)
        got = chip_trade(after(blocks, served), n_dev)
        first_ids = [got[:, t].reshape(n_chip * IDW) for t in range(n_tab)]
        got = got.reshape(n_chip, n_tab, IDW)
        rounds = (jnp.max(got[:, :, IDW - 1], axis=0) + SLOTS - 1) // SLOTS

        def more_ids(which, rnd, cid):
            return chip_exchange(id_blocks(which, rnd), cid, n_chip).reshape(n_chip * IDW)

        def own_slot(which, rnd):
            slot = round_slot(code_own[which], span, rnd, 0, SLOTS)
            return jnp.where(core == 0, slot, lax.rem(slot + n_chip * SLOTS, 2 * n_chip * SLOTS))

        def unpack(which, rnd, own):
            return unpack_rows(own_slot(which, rnd), own, swap_cores(own, n_dev), n_heads)

        def fetch_rest(which, first):
            def more(state):
                rnd, rows = state
                ids = more_ids(which, rnd, which)
                sent = owner_gather(ids, served, which, n_chip).reshape((n_chip, SLOTS) + tail)
                new = unpack(which, rnd, chip_exchange(sent, 2 + which, n_chip).reshape((n_chip * SLOTS,) + tail))
                now = lax.rem(code_own[which], span) // SLOTS == rnd
                return rnd + 1, jnp.where(jnp.repeat(now, row_width).reshape(rows.shape), new, rows)

            return lax.while_loop(lambda s: s[0] < rounds[which], more, (jnp.int32(1), first))[1]

        def packed(which, rnd, grad_own, grad_pair):
            plan = plans[which]
            dst = 2 * half_slot(plan, rnd, SLOTS, n_chip * SLOTS)
            return pack_rows(plan['pos'], dst, plan['size'], grad_own, grad_pair, n_chip)

        def pair_rows(grad_rows):
            return grad_rows, swap_cores(grad_rows, n_dev)

        def return_rest(which, first, pair):
            def more(state):
                rnd, total = state
                ids = more_ids(which, rnd, 4 + which)
                rec = chip_exchange(packed(which, rnd, *pair).reshape(n_chip, 2 * SLOTS, 128), 6 + which, n_chip)
                new = owner_scatter(ids, rec.reshape(n_chip * 2 * SLOTS, 128), rows_dev, place)
                return rnd + 1, [p + q for p, q in zip(total, new)]

            return lax.while_loop(lambda s: s[0] < rounds[which], more, (jnp.int32(1), list(first)))[1]

        x1 = layer_plain(x_start, w_up, w_down, 0)
        sent0 = owner_gather(after(first_ids[0], x1), served, 0, n_chip)
        fetched0 = chip_trade(sent0, n_dev)
        sent1 = owner_gather(after(first_ids[1], sent0), served, 1, n_chip)
        fetched1 = chip_trade(sent1, n_dev)
        m1, g1 = layer_table_head(after(x1, sent1), w_up, w_down, w_gate, 1, 0)
        e1 = fetch_rest(0, unpack(0, 0, fetched0))
        x2, h2, x3, a3, dz3, rows3 = layer_middle(x1, m1, g1, e1, d_out, w_up, w_down, w_gate, w_proj, 2)
        pair1 = pair_rows(rows3)
        h3 = last_up(x3, w_up, 3)
        sent1 = packed(1, 0, *pair1)
        returned1 = chip_trade(sent1, n_dev)
        e3 = unpack(1, 0, after(fetched1, sent1))
        e3 = fetch_rest(1, e3)
        c2 = back_table(after(d_out, sent1), h3, x3, a3, dz3, e3, w_up, w_down, w_gate, 3, 1)
        rows1 = back_plain(c2, h2, x2, g1, w_up, w_down, w_proj, 2, 0)
        pair0 = pair_rows(rows1)
        total1 = owner_scatter(first_ids[1], after(returned1, rows1), rows_dev, place)
        total1 = return_rest(1, total1, pair1)
        placed1 = place_trade(total1, n_dev)
        sent0 = packed(0, 0, pair0[0], after(pair0[1], total1[0]))
        returned0 = chip_trade(sent0, n_dev)
        x_end = last_down(after(x3, sent0), h3, a3, e3, w_down, w_proj, 3, 1)
        grads = finish_table([after(p, x_end) for p in placed1], None, 1, n_tab)
        total0 = owner_scatter(first_ids[0], after(returned0, x_end), rows_dev, place)
        total0 = return_rest(0, total0, pair0)
        grads = finish_table(place_exchange(total0, 8), grads, 0, n_tab)
        return x_end, grads

    return jax.shard_map(step, mesh=mesh, in_specs=(tok_spec, tok_spec, tab_spec, P(), P(), P(), P(), tab_spec),
                         out_specs=(tok_spec, tab_spec), check_vma=False)
```

```python
import jax
import jax.numpy as jnp
from jax import lax
from jax.experimental import pallas as pl
from jax.experimental.pallas import tpu as pltpu
from jax.sharding import PartitionSpec as P


EPS = 1e-6
C1 = 0.7978845608028654
C2 = C1 * 0.044715
BF16 = jnp.bfloat16
F32 = jnp.float32
VMEM_LIMIT = 62 * 1024 * 1024
MESH = pl.DeviceIdType.MESH
PLANE = 8
SLOTS = 336
IDW = 1024
UNROLL = 16
LANES = 128
COLS = 256
CHUNK = 512
TILE = 256
WIDE_TILE = 512

SMEM_SPEC = pl.BlockSpec(memory_space=pltpu.SMEM)
VMEM_SPEC = pl.BlockSpec(memory_space=pltpu.VMEM)
ANY_SPEC = pl.BlockSpec(memory_space=pl.ANY)


def local_params():
    return pltpu.CompilerParams(vmem_limit_bytes=VMEM_LIMIT)


def remote_params(cid):
    return pltpu.CompilerParams(vmem_limit_bytes=VMEM_LIMIT, collective_id=cid, has_side_effects=True)


def cost(us):
    return pl.CostEstimate(flops=int(us * 9e8), bytes_accessed=2**23, transcendentals=0)


def shape_of(shape, dtype):
    return jax.ShapeDtypeStruct(shape, dtype)


def gelu(x):
    half = 0.5 * x
    return half + half * jnp.tanh(x * (C1 + C2 * (x * x)))


def gelu_bwd(x, ct):
    x2 = x * x
    t = jnp.tanh(x * (C1 + C2 * x2))
    return ct * ((0.5 + 0.5 * t) + (x * (0.5 - (0.5 * t) * t)) * (C1 + (3 * C2) * x2))


def dot_nn(a, b):
    return jnp.dot(a, b, preferred_element_type=F32)


def dot_nt(a, b):
    return lax.dot_general(a, b, (((1,), (1,)), ((), ())), preferred_element_type=F32)


def rms(x_f):
    return lax.rsqrt(jnp.mean(x_f * x_f, axis=-1, keepdims=True) + EPS)


def pair_at(index):
    return pl.ds(pl.multiple_of(index, 2), 2)


def owner_gather(ids, served, which, n_src):
    work = gather_step(served, which, n_src)

    def kernel(ids_ref, served_ref, out_ref, *scratch):
        work((ids_ref, served_ref), out_ref, scratch)

    return pl.pallas_call(
        kernel, out_shape=gathered(served, n_src), in_specs=[SMEM_SPEC, ANY_SPEC], out_specs=VMEM_SPEC,
        scratch_shapes=gather_scratch(served), compiler_params=local_params(), name="owner_gather", cost_estimate=cost(14),
    )(ids, served)


def gathered(served, n_src):
    return shape_of((n_src * SLOTS, served.shape[3] // LANES, LANES), BF16)


def gather_scratch(served):
    blk, width = served.shape[2:]
    return [pltpu.VMEM((PLANE, blk, width), BF16), pltpu.VMEM((PLANE * blk * width // LANES + 8, LANES), F32),
            pltpu.SemaphoreType.DMA((PLANE,))]


def gather_step(served, which, n_src):
    blk, width = served.shape[2:]
    pieces = width // LANES

    def work(ins, out_ref, scratch):
        ids_ref, served_ref = ins
        native, flat, isem = scratch
        reads = [pltpu.make_async_copy(served_ref.at[b, which], native.at[b], isem.at[b]) for b in range(PLANE)]
        for c in reads:
            c.start()
        for b in range(PLANE):
            reads[b].wait()
            for c in range(pieces):
                flat[pl.ds(b * blk * pieces + c, blk, stride=pieces), :] = native[b, :, c * LANES:(c + 1) * LANES].astype(F32)

        def src(s, c):
            def part(b, c):
                for j in range(UNROLL):
                    r = b * UNROLL + j
                    out_ref[s * SLOTS + r] = flat[pair_at(ids_ref[s * IDW + r]), :].astype(BF16)
                return c

            lax.fori_loop(0, SLOTS // UNROLL, part, 0)
            return c

        lax.fori_loop(0, n_src, src, 0)

    return work


def token_kernel(body, tile, tokens, ins, weights, outs, scratch, us, extra_ins=(), extra_outs=(), first_step=None, mirror=None):
    steps = tokens // tile
    if mirror is not None:
        extra_outs = list(extra_outs) + [mirror[0]] * 2
        scratch = list(scratch) + [pltpu.VMEM((2, tile * mirror[1]) + mirror[0].shape[1:], mirror[0].dtype)] + [
            pltpu.SemaphoreType.DMA((steps,))] * 3
    ins = list(ins) + [(a, spec) for a, spec in extra_ins]
    outs = list(outs) + [(s, ANY_SPEC) for s in extra_outs]
    n_in, n_w, n_out = len(ins), len(weights), len(outs)
    n_own_in, n_own_out = n_in - len(extra_ins), n_out - len(extra_outs)

    def kernel(*refs):
        in_refs = refs[:n_in]
        w_hbm = refs[n_in:n_in + n_w]
        out_refs = refs[n_in + n_w:n_in + n_w + n_out]
        w_vmem = refs[n_in + n_w + n_out:n_in + 2 * n_w + n_out]
        sem = refs[n_in + 2 * n_w + n_out]
        rest = refs[n_in + 2 * n_w + n_out + 1:]
        copies = [pltpu.make_async_copy(w_hbm[i].at[weights[i][1]], w_vmem[i], sem.at[i]) for i in range(n_w)]
        opening = pl.program_id(0) == 0

        @pl.when(opening)
        def _():
            for c in copies:
                c.start()
            if first_step is not None:
                first_step(in_refs[n_own_in:], out_refs[n_own_out:], rest)

        def need(*which):
            @pl.when(opening)
            def _():
                for i in which:
                    copies[i].wait()

        if mirror is None:
            body(need, in_refs[:n_own_in], w_vmem, out_refs[:n_own_out], rest)
            return
        i = pl.program_id(0)
        other = lax.axis_index('emb') ^ 1
        barrier = pltpu.get_barrier_semaphore()
        own, pair = out_refs[-2:]
        stage, keep_sem, send_sem, recv_sem = rest[-4:]
        per = tile * mirror[1]

        def keep(j):
            return pltpu.make_async_copy(stage.at[lax.rem(j, 2)], own.at[pl.ds(j * per, per)], keep_sem.at[j])

        def send(j):
            return pltpu.make_async_remote_copy(
                src_ref=own.at[pl.ds(j * per, per)], dst_ref=pair.at[pl.ds(j * per, per)], send_sem=send_sem.at[j],
                recv_sem=recv_sem.at[j], device_id=(other,), device_id_type=MESH)

        @pl.when(opening)
        def _():
            pl.semaphore_signal(barrier, inc=1, device_id=(other,), device_id_type=MESH)
            pl.semaphore_wait(barrier, 1)

        body(need, in_refs[:n_own_in], w_vmem, out_refs[:n_own_out], list(rest[:-4]) + [stage.at[lax.rem(i, 2)]])
        keep(i).start()

        @pl.when(i > 0)
        def _():
            keep(i - 1).wait()
            send(i - 1).start()

        @pl.when(i == steps - 1)
        def _():
            keep(i).wait()
            send(i).start()
            for j in range(steps):
                send(j).wait()

    def tiled(shape, per):
        if isinstance(per, pl.BlockSpec):
            return per
        return pl.BlockSpec((tile * per,) + shape[1:], lambda i: (i,) + (0,) * (len(shape) - 1))

    in_specs = [tiled(a.shape, per) for a, per in ins] + [ANY_SPEC] * n_w
    out_specs = [tiled(s.shape, per) for s, per in outs]
    w_scratch = [pltpu.VMEM(w.shape[1:], w.dtype) for w, _ in weights]
    return pl.pallas_call(
        kernel, grid=(tokens // tile,), out_shape=[s for s, _ in outs], in_specs=in_specs, out_specs=out_specs,
        scratch_shapes=w_scratch + [pltpu.SemaphoreType.DMA((n_w,))] + list(scratch),
        compiler_params=local_params() if mirror is None else remote_params(mirror[2]), cost_estimate=cost(us),
    )(*[a for a, _ in ins], *[w for w, _ in weights])


def mlp_up(u, w_up, act, h_ref, chunk=CHUNK):
    for j in range(w_up.shape[1] // chunk):
        cols = slice(j * chunk, (j + 1) * chunk)
        h = dot_nn(u, w_up[:, cols]).astype(BF16)
        if h_ref is not None:
            h_ref[:, cols] = h
        if act is not None:
            act[:, cols] = gelu(h.astype(F32)).astype(BF16)


def store_rows(ref, value):
    tokens, width = value.shape
    n = width // LANES
    for c in range(n):
        ref[pl.ds(c, tokens, stride=n), :] = value[:, c * LANES:(c + 1) * LANES]


def layer_plain(x, w_up, w_down, layer, tile=WIDE_TILE):
    tokens, d = x.shape

    def body(need, ins, w, outs, rest):
        need(0, 1)
        x_f = ins[0][...].astype(F32)
        u = (x_f * rms(x_f)).astype(BF16)
        mlp_up(u, w[0], rest[0], None)
        for q in range(d // COLS):
            cols = slice(q * COLS, (q + 1) * COLS)
            m = dot_nn(rest[0][...], w[1][:, cols]).astype(BF16)
            outs[0][:, cols] = (ins[0][:, cols].astype(F32) + m.astype(F32)).astype(BF16)

    return token_kernel(body, tile, tokens, [(x, 1)], [(w_up, layer), (w_down, layer)],
                        [(shape_of(x.shape, BF16), 1)], [pltpu.VMEM((tile, w_up.shape[2]), BF16)], 44)[0]


def layer_table_head(x, w_up, w_down, w_gate, layer, which, ids, served, n_src, tile=WIDE_TILE):
    tokens, d = x.shape
    gather = gather_step(served, 1, n_src)
    sent = gathered(served, n_src)

    def first_step(ins, outs, rest):
        stage, sem = rest[-2:]
        gather(ins, stage, rest[1:-2])
        done = pltpu.make_async_copy(stage, outs[0], sem)
        done.start()
        done.wait()

    def body(need, ins, w, outs, rest):
        need(0, 1, 2)
        x_f = ins[0][...].astype(F32)
        u = (x_f * rms(x_f)).astype(BF16)
        mlp_up(u, w[0], rest[0], None)
        a = dot_nn(u, w[2][...]).astype(BF16)
        outs[1][...] = gelu(a.astype(F32)).astype(BF16)
        for q in range(d // COLS):
            cols = slice(q * COLS, (q + 1) * COLS)
            outs[0][:, cols] = dot_nn(rest[0][...], w[1][:, cols]).astype(BF16)

    return token_kernel(body, tile, tokens, [(x, 1)],
                        [(w_up, layer), (w_down, layer), (w_gate, which)],
                        [(shape_of(x.shape, BF16), 1), (shape_of(x.shape, BF16), 1)],
                        [pltpu.VMEM((tile, w_up.shape[2]), BF16)] + gather_scratch(served) +
                        [pltpu.VMEM(sent.shape, BF16), pltpu.SemaphoreType.DMA], 60,
                        [(ids, SMEM_SPEC), (served, ANY_SPEC)], [sent], first_step)


def layer_middle(x, m, g, e, d_out, w_up, w_down, w_gate, w_proj, layer, tile=TILE):
    tokens, d = x.shape
    ff = w_up.shape[2]

    def body(need, ins, w, outs, rest):
        x_ref, m_ref, g_ref, e_ref, c_ref = ins
        x2_ref, h_ref, x3_ref, a_ref, dz_ref, h3_ref = outs
        act = rest[0]
        need(4, 0)
        z = (g_ref[...].astype(F32) * e_ref[...].astype(F32)).astype(BF16)
        q = dot_nn(z, w[4][...]).astype(BF16)
        x2 = ((x_ref[...].astype(F32) + m_ref[...].astype(F32)) + q.astype(F32)).astype(BF16)
        x2_ref[...] = x2
        x_f = x2.astype(F32)
        u = (x_f * rms(x_f)).astype(BF16)
        need(1)
        mlp_up(u, w[0], act, h_ref)
        for n in range(d // COLS):
            cols = slice(n * COLS, (n + 1) * COLS)
            mm = dot_nn(act[...], w[1][:, cols]).astype(BF16)
            x3_ref[:, cols] = (x2_ref[:, cols].astype(F32) + mm.astype(F32)).astype(BF16)
        x_f = x3_ref[...].astype(F32)
        u = (x_f * rms(x_f)).astype(BF16)
        need(2, 3, 5)
        mlp_up(u, w[5], None, h3_ref)
        a = dot_nn(u, w[2][...]).astype(BF16)
        a_ref[...] = a
        gate = gelu(a.astype(F32)).astype(BF16)
        dz = dot_nt(c_ref[...], w[3][...])
        dz_ref[...] = dz
        store_rows(rest[-1], gate.astype(F32) * dz)

    vec = (shape_of((tokens, d), BF16), 1)
    return token_kernel(body, tile, tokens, [(x, 1), (m, 1), (g, 1), (e, 1), (d_out, 1)],
                        [(w_up, layer), (w_down, layer), (w_gate, 1), (w_proj, 1), (w_proj, 0), (w_up, layer + 1)],
                        [vec, (shape_of((tokens, ff), BF16), 1), vec, vec, (shape_of((tokens, d), F32), 1),
                         (shape_of((tokens, ff), BF16), 1)],
                        [pltpu.VMEM((tile, ff), BF16)], 90,
                        mirror=(shape_of((tokens * d // LANES, LANES), F32), d // LANES, 10))


def last_down(x, h, a, e, w_down, w_proj, layer, which, tile=TILE):
    tokens, d = x.shape
    ff = h.shape[1]

    def body(need, ins, w, outs, rest):
        x_ref, h_ref, a_ref, e_ref = ins
        act = rest[0]
        need(0, 1)
        gate = gelu(a_ref[...].astype(F32)).astype(BF16)
        z = (gate.astype(F32) * e_ref[...].astype(F32)).astype(BF16)
        for j in range(ff // CHUNK):
            cols = slice(j * CHUNK, (j + 1) * CHUNK)
            act[:, cols] = gelu(h_ref[:, cols].astype(F32)).astype(BF16)
        for n in range(d // COLS):
            cols = slice(n * COLS, (n + 1) * COLS)
            m = dot_nn(act[...], w[0][:, cols]).astype(BF16)
            q = dot_nn(z, w[1][:, cols]).astype(BF16)
            outs[0][:, cols] = ((x_ref[:, cols].astype(F32) + m.astype(F32)) + q.astype(F32)).astype(BF16)

    return token_kernel(body, tile, tokens, [(x, 1), (h, 1), (a, 1), (e, 1)],
                        [(w_down, layer), (w_proj, which)], [(shape_of(x.shape, BF16), 1)],
                        [pltpu.VMEM((tile, ff), BF16)], 30)[0]


def back_mlp(c_b, h_ref, w_up, w_down, dh):
    chunk = CHUNK
    for j in range(h_ref.shape[1] // chunk):
        cols = slice(j * chunk, (j + 1) * chunk)
        d_act = dot_nt(c_b, w_down[cols, :])
        dh[:, cols] = gelu_bwd(h_ref[:, cols].astype(F32), d_act).astype(BF16)
    return jnp.concatenate([dot_nt(dh[...], w_up[n * COLS:(n + 1) * COLS, :]) for n in range(w_up.shape[0] // COLS)], axis=1)


def back_norm(c_f, x_ref, du):
    x_f = x_ref[...].astype(F32)
    s = rms(x_f)
    return c_f + (s * du - x_f * (s * s * s) * jnp.mean(x_f * du, axis=-1, keepdims=True))


def back_table(c, h, x, a, dz, e, w_up, w_down, w_gate, layer, which, tile=TILE):
    tokens, d = x.shape
    ff = h.shape[1]

    def body(need, ins, w, outs, rest):
        c_ref, h_ref, x_ref, a_ref, dz_ref, e_ref = ins
        need(0, 1, 2)
        d_gate = gelu_bwd(a_ref[...].astype(F32), dz_ref[...] * e_ref[...].astype(F32)).astype(BF16)
        rest[1][...] = dot_nt(d_gate, w[2][...])
        du = back_mlp(c_ref[...], h_ref, w[0], w[1], rest[0]) + rest[1][...]
        outs[0][...] = back_norm(c_ref[...].astype(F32), x_ref, du)

    return token_kernel(body, tile, tokens,
                        [(c, 1), (h, 1), (x, 1), (a, 1), (dz, 1), (e, 1)],
                        [(w_up, layer), (w_down, layer), (w_gate, which)],
                        [(shape_of((tokens, d), F32), 1)],
                        [pltpu.VMEM((tile, ff), BF16), pltpu.VMEM((tile, d), F32)], 58)[0]


def back_plain(c, h, x, g, w_up, w_down, w_proj, layer, which, tile=TILE):
    tokens, d = x.shape
    ff = h.shape[1]

    def body(need, ins, w, outs, rest):
        c_ref, h_ref, x_ref, g_ref = ins
        need(0, 1, 2)
        du = back_mlp(c_ref[...].astype(BF16), h_ref, w[0], w[1], rest[0])
        c_low = back_norm(c_ref[...], x_ref, du).astype(BF16)
        store_rows(rest[-1], g_ref[...].astype(F32) * dot_nt(c_low, w[2][...]))

    return token_kernel(body, tile, tokens, [(c, 1), (h, 1), (x, 1), (g, 1)],
                        [(w_up, layer), (w_down, layer), (w_proj, which)], [],
                        [pltpu.VMEM((tile, ff), BF16)], 58,
                        mirror=(shape_of((tokens * d // LANES, LANES), F32), d // LANES, 11))


def split_rows(tables, place):
    n_tab, rows, width = tables.shape
    blk = rows // PLANE

    def kernel(place_ref, src, out, buf, isem, osem):
        reads = [pltpu.make_async_copy(src.at[t], buf.at[t], isem.at[t]) for t in range(n_tab)]
        for c in reads:
            c.start()
        writes = []
        for t in range(n_tab):
            reads[t].wait()
            for b in range(PLANE):
                writes.append(pltpu.make_async_copy(buf.at[t, pl.ds(b * blk, blk)], out.at[place_ref[0] ^ b, t], osem.at[t * PLANE + b]))
                writes[-1].start()
        for c in writes:
            c.wait()

    return pl.pallas_call(
        kernel, out_shape=shape_of((PLANE, n_tab, blk, width), tables.dtype), in_specs=[SMEM_SPEC, ANY_SPEC], out_specs=ANY_SPEC,
        scratch_shapes=[pltpu.VMEM(tables.shape, tables.dtype), pltpu.SemaphoreType.DMA((n_tab,)),
                        pltpu.SemaphoreType.DMA((n_tab * PLANE,))],
        compiler_params=local_params(), name="split_rows", cost_estimate=cost(4))(place, tables)


def make_ids(uid, start, count, peak, rnd, blank):
    n_tgt = count.shape[0]
    rows = -(-SLOTS // LANES)

    def kernel(uid_ref, start_ref, count_ref, peak_ref, rnd_ref, out_ref):
        lane = lax.broadcasted_iota(jnp.int32, (1, LANES), 1)
        out_ref[...] = jnp.full(out_ref.shape, peak_ref[0], jnp.int32)
        for g in range(n_tgt):
            shift = rnd_ref[0] * SLOTS
            left = jnp.clip(count_ref[g] - shift, 0, SLOTS)
            at = jnp.minimum(start_ref[g] + shift, (uid_ref.shape[0] - rows - 1) * LANES)
            row, off = at // LANES, lax.rem(at, LANES)
            turned = [pltpu.roll(uid_ref[row + i], lax.rem(LANES - off, LANES), axis=1) for i in range(rows + 1)]
            for i in range(rows):
                ids = jnp.where(lane < LANES - off, turned[i], turned[i + 1])
                out_ref[g, i:i + 1, :] = jnp.where(i * LANES + lane < left, ids, blank)

    return pl.pallas_call(
        kernel, out_shape=shape_of((n_tgt, IDW // LANES, LANES), jnp.int32),
        in_specs=[VMEM_SPEC] + [SMEM_SPEC] * 4, out_specs=VMEM_SPEC, compiler_params=local_params(), name="make_ids",
        cost_estimate=cost(3),
    )(uid, start, count, peak, jnp.reshape(rnd, (1,)).astype(jnp.int32))


def unpack_rows(idx, rec_own, rec_pair, heads):
    n = idx.shape[0]
    half, pieces = rec_own.shape[0], rec_own.shape[1]
    tokens, tile = n // heads, TILE
    per = heads * pieces

    def kernel(idx_ref, own_ref, pair_ref, out_ref, rec, stage, sem):
        copies = [pltpu.make_async_copy(own_ref, rec.at[pl.ds(0, half)], sem.at[0]),
                  pltpu.make_async_copy(pair_ref, rec.at[pl.ds(half, half)], sem.at[1])]
        for c in copies:
            c.start()
        for c in copies:
            c.wait()

        def part(i, c):
            def blk(b, c):
                for j in range(UNROLL):
                    row = rec[idx_ref[i * (tile * heads) + b * UNROLL + j]]
                    stage[pl.ds(pl.multiple_of(b * UNROLL * pieces, UNROLL * pieces) + pieces * j, pieces), :] = row.astype(F32)
                return c

            lax.fori_loop(0, tile * heads // UNROLL, blk, 0)
            for c in range(per):
                out_ref[pl.ds(i * tile, tile), c * LANES:(c + 1) * LANES] = stage[pl.ds(c, tile, stride=per), :].astype(BF16)
            return c

        lax.fori_loop(0, tokens // tile, part, 0)

    return pl.pallas_call(
        kernel, out_shape=shape_of((tokens, per * LANES), BF16),
        in_specs=[SMEM_SPEC, ANY_SPEC, ANY_SPEC], out_specs=VMEM_SPEC,
        scratch_shapes=[pltpu.VMEM((2 * half, pieces, LANES), BF16), pltpu.VMEM((tile * per, LANES), F32), pltpu.SemaphoreType.DMA((2,))],
        compiler_params=local_params(), name="unpack_rows", cost_estimate=cost(16),
    )(idx, rec_own, rec_pair)


def pack_rows(pos, dst, size, grad_own, grad_pair, n_tgt):
    n = grad_own.shape[0]
    n_row = 2 * n_tgt * SLOTS
    low = jnp.iinfo(jnp.int32).max

    def kernel(pos_ref, dst_ref, size_ref, own_ref, pair_ref, out_ref, g_ref, stage, sem):
        first = pltpu.make_async_copy(own_ref, g_ref.at[pl.ds(0, n)], sem.at[0])
        second = pltpu.make_async_copy(pair_ref, g_ref.at[pl.ds(n, n)], sem.at[1])
        first.start()
        second.start()
        first.wait()
        second.wait()

        def blk(b, acc):
            for j in range(UNROLL):
                p = pos_ref[b * UNROLL + j]
                row = g_ref[pair_at(p & low), :]
                acc = row + jnp.where(jnp.full((2, LANES), p, jnp.int32) < 0, acc, 0.0)
                stage[pair_at(dst_ref[b * UNROLL + j]), :] = acc
            return acc

        lax.fori_loop(0, (size_ref[0] + UNROLL - 1) // UNROLL, blk, jnp.zeros((2, LANES), F32))
        done = pltpu.make_async_copy(stage.at[pl.ds(0, n_row)], out_ref, sem.at[0])
        done.start()
        done.wait()

    return pl.pallas_call(
        kernel, out_shape=shape_of((n_row, LANES), F32),
        in_specs=[SMEM_SPEC, SMEM_SPEC, SMEM_SPEC, ANY_SPEC, ANY_SPEC], out_specs=ANY_SPEC,
        scratch_shapes=[pltpu.VMEM((2 * n, LANES), F32), pltpu.VMEM((n_row + 8, LANES), F32), pltpu.SemaphoreType.DMA((2,))],
        compiler_params=local_params(), name="pack_rows", cost_estimate=cost(26),
    )(pos, dst, size, grad_own, grad_pair)


def owner_scatter(ids, rec, rows, place):
    n_src = rec.shape[0] // (2 * SLOTS)
    per = UNROLL

    blk_rows = 2 * rows // PLANE

    def kernel(ids_ref, place_ref, rec_ref, *refs):
        outs, (acc, buf, sem, osem) = refs[:PLANE], refs[PLANE:]
        reads = [pltpu.make_async_copy(rec_ref.at[pl.ds(s * 2 * SLOTS, 2 * SLOTS)], buf.at[pl.ds(s * 2 * SLOTS, 2 * SLOTS)], sem.at[s])
                 for s in range(n_src)]
        for c in reads:
            c.start()

        def zero(i, c):
            acc[pl.ds(i * LANES, LANES), :] = jnp.zeros((LANES, LANES), F32)
            return c

        lax.fori_loop(0, 2 * rows // LANES, zero, 0)
        for c in reads:
            c.wait()

        def src(s, c):
            def blk(b, c):
                at = [pair_at(ids_ref[s * IDW + b * per + j]) for j in range(per)]
                base = pl.multiple_of((s * SLOTS + b * per) * 2, 2 * per)
                new = [acc[i, :] + buf[pl.ds(base + 2 * j, 2), :] for j, i in enumerate(at)]
                for i, v in zip(at, new):
                    acc[i, :] = v
                return c

            lax.fori_loop(0, SLOTS // per, blk, 0)
            return c

        lax.fori_loop(0, n_src, src, 0)
        writes = []
        for b in range(PLANE):
            at = pl.multiple_of((place_ref[0] ^ b) * blk_rows, blk_rows)
            writes.append(pltpu.make_async_copy(acc.at[pl.ds(at, blk_rows)], outs[b], osem.at[b]))
            writes[-1].start()
        for c in writes:
            c.wait()

    return pl.pallas_call(
        kernel, out_shape=[shape_of((blk_rows, LANES), F32)] * PLANE, in_specs=[SMEM_SPEC, SMEM_SPEC, ANY_SPEC],
        out_specs=[ANY_SPEC] * PLANE,
        scratch_shapes=[pltpu.VMEM((2 * rows + 8, LANES), F32), pltpu.VMEM((n_src * 2 * SLOTS, LANES), F32),
                        pltpu.SemaphoreType.DMA((n_src,)), pltpu.SemaphoreType.DMA((PLANE,))],
        compiler_params=local_params(), name="owner_scatter", cost_estimate=cost(20),
    )(ids, place, rec)


def finish_table(blocks, grads, which, n_tab):
    blk_rows = blocks[0].shape[0]
    blk = blk_rows // 2
    shape = (n_tab, PLANE * blk, COLS)
    first = grads is None

    def kernel(*refs):
        out, buf, stage, isem, osem = refs[-5:]
        reads = [pltpu.make_async_copy(refs[b], buf.at[b], isem.at[b]) for b in range(PLANE)]
        for c in reads:
            c.start()
        writes = []
        for b in range(PLANE):
            reads[b].wait()
            for c in range(2):
                stage[b, :, c * LANES:(c + 1) * LANES] = buf[b, pl.ds(c, blk, stride=2), :]
            writes.append(pltpu.make_async_copy(stage.at[b], out.at[which, pl.ds(b * blk, blk)], osem.at[b]))
            writes[-1].start()
        for c in writes:
            c.wait()

    args = list(blocks) + ([] if first else [grads])
    return pl.pallas_call(
        kernel, out_shape=shape_of(shape, F32), in_specs=[ANY_SPEC] * len(args), out_specs=ANY_SPEC,
        scratch_shapes=[pltpu.VMEM((PLANE, blk_rows, LANES), F32), pltpu.VMEM((PLANE, blk, COLS), F32),
                        pltpu.SemaphoreType.DMA((PLANE,)), pltpu.SemaphoreType.DMA((PLANE,))],
        input_output_aliases={} if first else {PLANE: 0},
        compiler_params=local_params(), name="finish_table", cost_estimate=cost(8))(*args)


def swap_cores(x, n_dev):
    return lax.ppermute(x, 'emb', [(i, i ^ 1) for i in range(n_dev)])


def chip_trade(x, n_dev):
    groups = [list(range(c, n_dev, 2)) for c in range(2)]
    return lax.all_to_all(x, 'emb', 0, 0, axis_index_groups=groups, tiled=True)


def chip_exchange(blocks, cid, n_chip):
    def kernel(x_ref, o_ref, ssem, rsem, lsem):
        me = lax.axis_index('emb')
        chip = me // 2
        barrier = pltpu.get_barrier_semaphore()
        for d in range(1, n_chip):
            pl.semaphore_signal(barrier, inc=1, device_id=(me ^ (2 * d),), device_id_type=MESH)
        pl.semaphore_wait(barrier, n_chip - 1)
        copies = [pltpu.make_async_copy(x_ref.at[chip], o_ref.at[chip], lsem)]
        for d in range(1, n_chip):
            copies.append(pltpu.make_async_remote_copy(
                src_ref=x_ref.at[chip ^ d], dst_ref=o_ref.at[chip], send_sem=ssem.at[d], recv_sem=rsem.at[d],
                device_id=(me ^ (2 * d),), device_id_type=MESH))
        for c in copies:
            c.start()
        for c in copies:
            c.wait()

    return pl.pallas_call(
        kernel, out_shape=shape_of(blocks.shape, blocks.dtype), in_specs=[ANY_SPEC], out_specs=ANY_SPEC,
        scratch_shapes=[pltpu.SemaphoreType.DMA((n_chip,)), pltpu.SemaphoreType.DMA((n_chip,)), pltpu.SemaphoreType.DMA],
        compiler_params=remote_params(cid), name="chip_exchange", cost_estimate=cost(100))(blocks)


def plane_trade(x, n_dev):
    groups = [list(range(z, z + PLANE)) for z in range(0, n_dev, PLANE)]
    return lax.all_to_all(x, 'emb', 0, 0, axis_index_groups=groups, tiled=True)


def place_trade(blocks, n_dev):
    return [blocks[0]] + [lax.ppermute(blocks[b], 'emb', [(i, i ^ b) for i in range(n_dev)]) for b in range(1, PLANE)]


def place_exchange(blocks, cid):
    def kernel(*refs):
        srcs, outs, (ssem, rsem) = refs[:PLANE - 1], refs[PLANE - 1:2 * (PLANE - 1)], refs[-2:]
        me = lax.axis_index('emb')
        barrier = pltpu.get_barrier_semaphore()
        for b in range(1, PLANE):
            pl.semaphore_signal(barrier, inc=1, device_id=(me ^ b,), device_id_type=MESH)
        pl.semaphore_wait(barrier, PLANE - 1)
        copies = [pltpu.make_async_remote_copy(
            src_ref=srcs[b - 1], dst_ref=outs[b - 1], send_sem=ssem.at[b], recv_sem=rsem.at[b],
            device_id=(me ^ b,), device_id_type=MESH) for b in range(1, PLANE)]
        for c in copies:
            c.start()
        for c in copies:
            c.wait()

    shape = shape_of(blocks[0].shape, blocks[0].dtype)
    got = pl.pallas_call(
        kernel, out_shape=[shape] * (PLANE - 1), in_specs=[ANY_SPEC] * (PLANE - 1), out_specs=[ANY_SPEC] * (PLANE - 1),
        scratch_shapes=[pltpu.SemaphoreType.DMA((PLANE,)), pltpu.SemaphoreType.DMA((PLANE,))],
        compiler_params=remote_params(cid), name="place_exchange", cost_estimate=cost(50))(*blocks[1:])
    return [blocks[0]] + list(got)


def after(x, *deps):
    return lax.optimization_barrier((x,) + deps)[0]


def sort_requests(ids_pair, rows_dev, n_dev):
    n = ids_pair.shape[0]
    n_chip = n_dev // 2
    blk = rows_dev // PLANE
    owner, local = ids_pair // rows_dev, lax.rem(ids_pair, rows_dev)
    server = owner ^ (local // blk)
    name = (lax.rem(server, 2) * n_chip + server // 2) * rows_dev + lax.rem(owner, PLANE) * blk + lax.rem(local, blk)
    return lax.sort(name * n + jnp.arange(n, dtype=jnp.int32))


def route_plan(key, n_own, rows_dev, n_dev, me):
    n = key.shape[0]
    n_chip = n_dev // 2
    sid, pos = key // n, lax.rem(key, n)
    n_low = jnp.sum((sid < n_chip * rows_dev).astype(jnp.int32))
    first = sid != jnp.concatenate([jnp.full((1,), -1, jnp.int32), sid[:-1]])
    slot = jnp.cumsum(first.astype(jnp.int32)) - 1
    tgt = sid // rows_dev
    bound = jnp.arange(n_dev + 1, dtype=jnp.int32)
    start = jnp.sum((first[None, :] & (tgt[None, :] < bound[:, None])).astype(jnp.int32), axis=1)
    rank = slot - jnp.sum(jnp.where(tgt[None, :] == bound[:-1, None], start[:-1, None], 0), axis=0)
    code = tgt * (2 * rows_dev) + rank
    count = start[1:] - start[:-1]
    core = lax.rem(me, 2)
    size = jnp.where(core == 0, n_low, n - n_low)
    begin = jnp.where(core == 0, 0, n_low)
    low = jnp.iinfo(jnp.int32).min
    both = jnp.stack([2 * pos + jnp.where(first, 0, low), code])
    both = jnp.concatenate([both, both, both[:, :UNROLL]], axis=1)
    mine = lax.dynamic_slice(both, (0, begin), (2, n + UNROLL))
    valid = jnp.arange(n + UNROLL, dtype=jnp.int32) < size
    most = jnp.iinfo(jnp.int32).max
    distinct = jnp.where(first & (sid // (n_chip * rows_dev) == core), sid, most)
    start = lax.dynamic_slice(start, (core * n_chip,), (n_chip,))
    return dict(pos=jnp.where(valid, mine[0], 0), code=jnp.where(valid, mine[1], -1), distinct=distinct, start=start - start[0],
                size=size.reshape(1), by_pos=jnp.where(pos < n_own, pos * (n_dev * 2 * rows_dev) + code, most),
                count=lax.dynamic_slice(count, (core * n_chip,), (n_chip,)), peak=jnp.max(count).reshape(1))


def round_slot(code, span, rnd, trash, width):
    tgt, rank = code // span, lax.rem(code, span) - rnd * SLOTS
    inside = (code >= 0) & (rank >= 0) & (rank < SLOTS)
    return jnp.where(inside, tgt * width + rank, trash)


def solution(mesh):
    n_dev = mesh.shape['emb']
    n_chip = n_dev // 2
    tok_spec = P('emb', None)
    tab_spec = P(None, 'emb', None)

    def step(x_start, d_out, token_ids, w_up, w_down, w_gate, w_proj, tables):
        n_tab, n_tok, n_heads = token_ids.shape
        rows_dev, row_width = tables.shape[1], tables.shape[2]
        n_req = n_tok * n_heads
        tail = (row_width // LANES, LANES)
        me = lax.axis_index('emb')
        core = lax.rem(me, 2)

        flat_ids = token_ids.reshape(n_tab, n_req)
        ids_pair = jnp.concatenate([flat_ids, swap_cores(flat_ids, n_dev)], axis=1)
        place = lax.rem(me, PLANE).reshape(1)
        split = split_rows(tables, place)
        served = plane_trade(split, n_dev)
        keys = [sort_requests(after(ids_pair, split)[t], rows_dev, n_dev) for t in range(n_tab)]

        plans = [route_plan(keys[t], n_req, rows_dev, n_dev, me) for t in range(n_tab)]
        distinct = lax.sort(jnp.stack([plan['distinct'] for plan in plans]), dimension=1)
        x1 = layer_plain(after(x_start, *[plan['distinct'] for plan in plans]), w_up, w_down, 0)
        margin = jnp.zeros((n_tab, CHUNK), jnp.int32)
        distinct = jnp.concatenate([2 * lax.rem(distinct, rows_dev), margin], axis=1).reshape(n_tab, -1, 1, LANES)
        span = 2 * rows_dev
        in_order = lax.sort(after(jnp.stack([plan['by_pos'] for plan in plans]), distinct), dimension=1)
        code_own = lax.rem(in_order[:, :n_req], n_dev * span)

        def half_slot(plan, rnd, width, trash):
            code = plan['code']
            code = jnp.where(code >= 0, lax.rem(code, n_chip * span), code)
            return round_slot(code, span, rnd, trash, width)

        def id_blocks(which, rnd):
            plan = plans[which]
            return make_ids(distinct[which], plan['start'], plan['count'], plan['peak'], rnd, 2 * rows_dev)

        blocks = jnp.stack([id_blocks(t, jnp.int32(0)) for t in range(n_tab)], axis=1)
        blocks = blocks.reshape(n_chip, n_tab * IDW // LANES, LANES)
        got = chip_exchange(after(blocks, served, x1), 9, n_chip).reshape(n_chip, n_tab, IDW)
        first_ids = [got[:, t].reshape(n_chip * IDW) for t in range(n_tab)]
        rounds = [(jnp.max(got[:, t, IDW - 1]) + SLOTS - 1) // SLOTS for t in range(n_tab)]

        def more_ids(which, rnd, cid):
            return chip_exchange(id_blocks(which, rnd), cid, n_chip).reshape(n_chip * IDW)

        def own_slot(which, rnd):
            slot = round_slot(code_own[which], span, rnd, 0, SLOTS)
            return jnp.where(core == 0, slot, lax.rem(slot + n_chip * SLOTS, 2 * n_chip * SLOTS))

        def unpack(which, rnd, own):
            return unpack_rows(own_slot(which, rnd), own, swap_cores(own, n_dev), n_heads)

        def fetch_rest(which, first):
            def more(state):
                rnd, rows = state
                ids = more_ids(which, rnd, which)
                sent = owner_gather(ids, served, which, n_chip).reshape((n_chip, SLOTS) + tail)
                new = unpack(which, rnd, chip_exchange(sent, 2 + which, n_chip).reshape((n_chip * SLOTS,) + tail))
                now = lax.rem(code_own[which], span) // SLOTS == rnd
                return rnd + 1, jnp.where(jnp.repeat(now, row_width).reshape(rows.shape), new, rows)

            return lax.while_loop(lambda s: s[0] < rounds[which], more, (jnp.int32(1), first))[1]

        def packed(which, rnd, grad_own, grad_pair):
            plan = plans[which]
            dst = 2 * half_slot(plan, rnd, SLOTS, n_chip * SLOTS)
            return pack_rows(plan['pos'], dst, plan['size'], grad_own, grad_pair, n_chip)

        def return_rest(which, first, pair):
            def more(state):
                rnd, total = state
                ids = more_ids(which, rnd, 4 + which)
                rec = chip_exchange(packed(which, rnd, *pair).reshape(n_chip, 2 * SLOTS, LANES), 6 + which, n_chip)
                new = owner_scatter(ids, rec.reshape(n_chip * 2 * SLOTS, LANES), rows_dev, place)
                return rnd + 1, [p + q for p, q in zip(total, new)]

            return lax.while_loop(lambda s: s[0] < rounds[which], more, (jnp.int32(1), list(first)))[1]

        sent0 = owner_gather(first_ids[0], served, 0, n_chip)
        fetched0 = chip_trade(sent0, n_dev)
        m1, g1, sent1 = layer_table_head(after(x1, sent0), w_up, w_down, w_gate, 1, 0, first_ids[1], served, n_chip)
        e1 = fetch_rest(0, unpack(0, 0, fetched0))
        fetched1 = chip_trade(after(sent1, e1), n_dev)
        x2, h2, x3, a3, dz3, h3, *pair1 = layer_middle(x1, m1, g1, e1, d_out, w_up, w_down, w_gate, w_proj, 2)
        sent1 = packed(1, 0, *pair1)
        returned1 = chip_trade(after(sent1, fetched1), n_dev)
        e3 = unpack(1, 0, after(fetched1, sent1))
        e3 = fetch_rest(1, e3)
        c2 = back_table(after(d_out, sent1), h3, x3, a3, dz3, e3, w_up, w_down, w_gate, 3, 1)
        pair0 = back_plain(c2, h2, x2, g1, w_up, w_down, w_proj, 2, 0)
        sent0 = packed(0, 0, *pair0)
        returned0 = chip_trade(after(sent0, returned1), n_dev)
        total1 = owner_scatter(first_ids[1], after(returned1, sent0), rows_dev, place)
        total1 = return_rest(1, total1, pair1)
        placed1 = place_trade(total1, n_dev)
        x_end = last_down(after(x3, *total1), h3, a3, e3, w_down, w_proj, 3, 1)
        grads = finish_table([after(p, x_end) for p in placed1], None, 1, n_tab)
        total0 = owner_scatter(first_ids[0], after(returned0, x_end), rows_dev, place)
        total0 = return_rest(0, total0, pair0)
        grads = finish_table(place_exchange(total0, 8), grads, 0, n_tab)
        return x_end, grads

    return jax.shard_map(step, mesh=mesh, in_specs=(tok_spec, tok_spec, tab_spec, P(), P(), P(), P(), tab_spec),
                         out_specs=(tok_spec, tab_spec), check_vma=False)
```

```python
import jax
import jax.numpy as jnp
from jax import lax
from jax.experimental import pallas as pl
from jax.experimental.pallas import tpu as pltpu
from jax.sharding import PartitionSpec as P


EPS = 1e-6
C1 = 0.7978845608028654
C2 = C1 * 0.044715
BF16 = jnp.bfloat16
I32 = jnp.iinfo(jnp.int32)
F32 = jnp.float32
VMEM_LIMIT = 62 * 1024 * 1024
MESH = pl.DeviceIdType.MESH
PLANE = 8
SLOTS = 336
IDW = 1024
UNROLL = 16
LANES = 128
COLS = 256
CHUNK = 512
TILE = 256
WIDE_TILE = 512

SMEM_SPEC = pl.BlockSpec(memory_space=pltpu.SMEM)
VMEM_SPEC = pl.BlockSpec(memory_space=pltpu.VMEM)
ANY_SPEC = pl.BlockSpec(memory_space=pl.ANY)


def local_params():
    return pltpu.CompilerParams(vmem_limit_bytes=VMEM_LIMIT)


def remote_params(cid):
    return pltpu.CompilerParams(vmem_limit_bytes=VMEM_LIMIT, collective_id=cid, has_side_effects=True)


def cost(us):
    return pl.CostEstimate(flops=int(us * 9e8), bytes_accessed=2**23, transcendentals=0)


def shape_of(shape, dtype):
    return jax.ShapeDtypeStruct(shape, dtype)


def gelu(x):
    half = 0.5 * x
    return half + half * jnp.tanh(x * (C1 + C2 * (x * x)))


def gelu_bwd(x, ct):
    x2 = x * x
    t = jnp.tanh(x * (C1 + C2 * x2))
    return ct * ((0.5 + 0.5 * t) + (x * (0.5 - (0.5 * t) * t)) * (C1 + (3 * C2) * x2))


def dot_nn(a, b):
    return jnp.dot(a, b, preferred_element_type=F32)


def dot_nt(a, b):
    return lax.dot_general(a, b, (((1,), (1,)), ((), ())), preferred_element_type=F32)


def rms(x_f):
    return lax.rsqrt(jnp.mean(x_f * x_f, axis=-1, keepdims=True) + EPS)


def pair_at(index):
    return pl.ds(pl.multiple_of(index, 2), 2)


def owner_gather(ids, served, which, n_src):
    work = gather_step(served, which, n_src)

    def kernel(ids_ref, served_ref, out_ref, *scratch):
        work((ids_ref, served_ref), out_ref, scratch, lambda: None)

    return pl.pallas_call(
        kernel, out_shape=gathered(served, n_src), in_specs=[SMEM_SPEC, ANY_SPEC], out_specs=VMEM_SPEC,
        scratch_shapes=gather_scratch(served), compiler_params=local_params(), name="owner_gather", cost_estimate=cost(14),
    )(ids, served)


def gathered(served, n_src):
    return shape_of((n_src * SLOTS, served.shape[3] // LANES, LANES), BF16)


def gather_scratch(served):
    blk, width = served.shape[2:]
    return [pltpu.VMEM((PLANE, blk, width), BF16), pltpu.VMEM((PLANE * blk * width // LANES + 8, LANES), F32),
            pltpu.SemaphoreType.DMA((PLANE,))]


def gather_step(served, which, n_src):
    blk, width = served.shape[2:]
    pieces = width // LANES

    def work(ins, out_ref, scratch, then):
        ids_ref, served_ref = ins
        native, flat, isem = scratch
        reads = [pltpu.make_async_copy(served_ref.at[b, which], native.at[b], isem.at[b]) for b in range(PLANE)]
        for c in reads:
            c.start()
        for b in range(PLANE):
            reads[b].wait()
            for c in range(pieces):
                flat[pl.ds(b * blk * pieces + c, blk, stride=pieces), :] = native[b, :, c * LANES:(c + 1) * LANES].astype(F32)
        then()

        def src(s, c):
            def part(b, c):
                for j in range(UNROLL):
                    r = b * UNROLL + j
                    out_ref[s * SLOTS + r] = flat[pair_at(ids_ref[s * IDW + r]), :].astype(BF16)
                return c

            lax.fori_loop(0, SLOTS // UNROLL, part, 0)
            return c

        lax.fori_loop(0, n_src, src, 0)

    return work


def unpacked(idx, rec, heads):
    return shape_of((idx.shape[0] // heads, heads * rec.shape[1] * LANES), BF16)


def unpack_scratch(rec, heads):
    half, pieces = rec.shape[0], rec.shape[1]
    rows = pltpu.VMEM((TILE * heads * pieces, LANES), F32)
    return [pltpu.VMEM((2 * half + 8, pieces, LANES), BF16), rows, pltpu.SemaphoreType.DMA((2,)), rows,
            pltpu.VMEM((TILE, heads * pieces * LANES), BF16)]


def unpack_step(idx, rec_own, rec_pair, heads):
    n = idx.shape[0]
    half, pieces = rec_own.shape[0], rec_own.shape[1]
    per = heads * pieces

    def work(ins, out_ref, scratch, then):
        idx_ref, own_ref, pair_ref = ins[:3]
        rec, stage, sem, more, native = scratch
        copies = [pltpu.make_async_copy(own_ref, rec.at[pl.ds(0, half)], sem.at[0]),
                  pltpu.make_async_copy(pair_ref, rec.at[pl.ds(half, half)], sem.at[1])]
        for c in copies:
            c.start()
        for c in copies:
            c.wait()
        then()

        def part(i, c):
            first = i * (TILE * heads)

            def blk(b, c):
                for j in range(UNROLL):
                    row = rec[idx_ref[first + b * UNROLL + j]]
                    stage[pl.ds(pl.multiple_of(b * UNROLL * pieces, UNROLL * pieces) + pieces * j, pieces), :] = row.astype(F32)
                return c

            lax.fori_loop(0, TILE * heads // UNROLL, blk, 0)
            if len(ins) > 3:
                late_ref, rounds_ref = ins[3:]

                @pl.when(rounds_ref[0] > 1)
                def _():
                    fetch = pltpu.make_async_copy(late_ref.at[pl.ds(i * TILE, TILE)], native, sem.at[0])
                    fetch.start()
                    fetch.wait()
                    store_rows(more, native[...].astype(F32))

                    def patch(r, c):
                        @pl.when(idx_ref[first + r] == 2 * half)
                        def _():
                            stage[pair_at(2 * r), :] = more[pair_at(2 * r), :]

                        return c

                    lax.fori_loop(0, TILE * heads, patch, 0)
            for c in range(per):
                out_ref[pl.ds(i * TILE, TILE), c * LANES:(c + 1) * LANES] = stage[pl.ds(c, TILE, stride=per), :].astype(BF16)
            return c

        lax.fori_loop(0, n // heads // TILE, part, 0)

    return work


def token_kernel(body, tile, tokens, ins, weights, outs, scratch, us, extra_ins=(), extra_outs=(), first_step=None, mirror=None):
    steps = tokens // tile
    if mirror is not None:
        extra_outs = list(extra_outs) + [mirror[0]] * 2
        scratch = list(scratch) + [pltpu.VMEM((2, tile * mirror[1]) + mirror[0].shape[1:], mirror[0].dtype)] + [
            pltpu.SemaphoreType.DMA((steps,))] * 3
    ins = list(ins) + [(a, spec) for a, spec in extra_ins]
    outs = list(outs) + [(s, ANY_SPEC) for s in extra_outs]
    n_in, n_w, n_out = len(ins), len(weights), len(outs)
    n_own_in, n_own_out = n_in - len(extra_ins), n_out - len(extra_outs)

    def kernel(*refs):
        in_refs = refs[:n_in]
        w_hbm = refs[n_in:n_in + n_w]
        out_refs = refs[n_in + n_w:n_in + n_w + n_out]
        w_vmem = refs[n_in + n_w + n_out:n_in + 2 * n_w + n_out]
        sem = refs[n_in + 2 * n_w + n_out]
        rest = refs[n_in + 2 * n_w + n_out + 1:]
        copies = [pltpu.make_async_copy(w_hbm[i].at[weights[i][1]], w_vmem[i], sem.at[i]) for i in range(n_w)]
        opening = pl.program_id(0) == 0

        @pl.when(opening)
        def _():
            def start_weights():
                for c in copies:
                    c.start()

            if first_step is None:
                start_weights()
            else:
                first_step(in_refs[n_own_in:], out_refs[n_own_out:], rest, start_weights)

        def need(*which):
            @pl.when(opening)
            def _():
                for i in which or range(n_w):
                    copies[i].wait()

        if mirror is None:
            body(need, in_refs[:n_own_in], w_vmem, out_refs[:n_own_out], rest)
            return
        i = pl.program_id(0)
        other = lax.axis_index('emb') ^ 1
        barrier = pltpu.get_barrier_semaphore()
        own, pair = out_refs[-2:]
        stage, keep_sem, send_sem, recv_sem = rest[-4:]
        per = tile * mirror[1]

        def keep(j):
            return pltpu.make_async_copy(stage.at[lax.rem(j, 2)], own.at[pl.ds(j * per, per)], keep_sem.at[j])

        def send(j):
            return pltpu.make_async_remote_copy(
                src_ref=own.at[pl.ds(j * per, per)], dst_ref=pair.at[pl.ds(j * per, per)], send_sem=send_sem.at[j],
                recv_sem=recv_sem.at[j], device_id=(other,), device_id_type=MESH)

        @pl.when(opening)
        def _():
            pl.semaphore_signal(barrier, inc=1, device_id=(other,), device_id_type=MESH)
            pl.semaphore_wait(barrier, 1)

        body(need, in_refs[:n_own_in], w_vmem, out_refs[:n_own_out], list(rest[:-4]) + [stage.at[lax.rem(i, 2)]])
        keep(i).start()

        @pl.when(i > 0)
        def _():
            keep(i - 1).wait()
            send(i - 1).start()

        @pl.when(i == steps - 1)
        def _():
            keep(i).wait()
            send(i).start()
            for j in range(steps):
                send(j).wait()

    def tiled(shape, per):
        if isinstance(per, pl.BlockSpec):
            return per
        return pl.BlockSpec((tile * per,) + shape[1:], lambda i: (i,) + (0,) * (len(shape) - 1))

    in_specs = [tiled(a.shape, per) for a, per in ins] + [ANY_SPEC] * n_w
    out_specs = [tiled(s.shape, per) for s, per in outs]
    w_scratch = [pltpu.VMEM(w.shape[1:], w.dtype) for w, _ in weights]
    return pl.pallas_call(
        kernel, grid=(tokens // tile,), out_shape=[s for s, _ in outs], in_specs=in_specs, out_specs=out_specs,
        scratch_shapes=w_scratch + [pltpu.SemaphoreType.DMA((n_w,))] + list(scratch),
        compiler_params=local_params() if mirror is None else remote_params(mirror[2]), cost_estimate=cost(us),
    )(*[a for a, _ in ins], *[w for w, _ in weights])


def mlp_up(u, w_up, act, h_ref, chunk=CHUNK):
    for j in range(w_up.shape[1] // chunk):
        cols = slice(j * chunk, (j + 1) * chunk)
        h = dot_nn(u, w_up[:, cols]).astype(BF16)
        if h_ref is not None:
            h_ref[:, cols] = h
        if act is not None:
            act[:, cols] = gelu(h.astype(F32)).astype(BF16)


def store_rows(ref, value):
    tokens, width = value.shape
    n = width // LANES
    for c in range(n):
        ref[pl.ds(c, tokens, stride=n), :] = value[:, c * LANES:(c + 1) * LANES]


def tile_of(ref, tile):
    return ref.at[pl.ds(pl.multiple_of(pl.program_id(0) * tile, tile), tile), :]


def unpack_ins(rows):
    return list(zip(rows, [SMEM_SPEC, ANY_SPEC, ANY_SPEC, ANY_SPEC, SMEM_SPEC]))


def layer_plain(x, w_up, w_down, layer, tile=WIDE_TILE):
    tokens, d = x.shape

    def body(need, ins, w, outs, rest):
        need()
        up, down = w
        x_f = ins[0][...].astype(F32)
        u = (x_f * rms(x_f)).astype(BF16)
        mlp_up(u, up, rest[0], None)
        for q in range(d // COLS):
            cols = slice(q * COLS, (q + 1) * COLS)
            m = dot_nn(rest[0][...], down[:, cols]).astype(BF16)
            outs[0][:, cols] = (ins[0][:, cols].astype(F32) + m.astype(F32)).astype(BF16)

    return token_kernel(body, tile, tokens, [(x, 1)], [(w_up, layer), (w_down, layer)],
                        [(shape_of(x.shape, BF16), 1)], [pltpu.VMEM((tile, w_up.shape[2]), BF16)], 44)[0]


def layer_table_head(x, w_up, w_down, w_gate, layer, which, ids, served, n_src, tile=WIDE_TILE):
    tokens, d = x.shape
    gather = gather_step(served, 1, n_src)
    sent = gathered(served, n_src)

    def first_step(ins, outs, rest, then):
        stage, sem = rest[-2:]
        gather(ins, stage, rest[1:-2], then)
        done = pltpu.make_async_copy(stage, outs[0], sem)
        done.start()
        done.wait()

    def body(need, ins, w, outs, rest):
        need()
        up, down, gate = w
        x_f = ins[0][...].astype(F32)
        u = (x_f * rms(x_f)).astype(BF16)
        mlp_up(u, up, rest[0], None)
        a = dot_nn(u, gate[...]).astype(BF16)
        outs[1][...] = gelu(a.astype(F32)).astype(BF16)
        for q in range(d // COLS):
            cols = slice(q * COLS, (q + 1) * COLS)
            outs[0][:, cols] = dot_nn(rest[0][...], down[:, cols]).astype(BF16)

    return token_kernel(body, tile, tokens, [(x, 1)],
                        [(w_up, layer), (w_down, layer), (w_gate, which)],
                        [(shape_of(x.shape, BF16), 1), (shape_of(x.shape, BF16), 1)],
                        [pltpu.VMEM((tile, w_up.shape[2]), BF16)] + gather_scratch(served) +
                        [pltpu.VMEM(sent.shape, BF16), pltpu.SemaphoreType.DMA], 60,
                        [(ids, SMEM_SPEC), (served, ANY_SPEC)], [sent], first_step)


def layer_middle(x, m, g, rows, d_out, w_up, w_down, w_gate, w_proj, layer, heads, tile=TILE):
    tokens, d = x.shape
    ff = w_up.shape[2]
    unpack = unpack_step(*rows[:3], heads)

    def body(need, ins, w, outs, rest):
        x_ref, m_ref, g_ref, c_ref = ins
        x2_ref, h_ref, x3_ref, a_ref, dz_ref, row_ref = outs
        act, e = rest[:2]
        need(4, 0)
        z = (g_ref[...].astype(F32) * tile_of(e, tile)[...].astype(F32)).astype(BF16)
        q = dot_nn(z, w[4][...]).astype(BF16)
        x2 = ((x_ref[...].astype(F32) + m_ref[...].astype(F32)) + q.astype(F32)).astype(BF16)
        x2_ref[...] = x2
        x_f = x2.astype(F32)
        u = (x_f * rms(x_f)).astype(BF16)
        need(1)
        mlp_up(u, w[0], act, h_ref)
        for n in range(d // COLS):
            cols = slice(n * COLS, (n + 1) * COLS)
            mm = dot_nn(act[...], w[1][:, cols]).astype(BF16)
            x3_ref[:, cols] = (x2_ref[:, cols].astype(F32) + mm.astype(F32)).astype(BF16)
        x_f = x3_ref[...].astype(F32)
        u = (x_f * rms(x_f)).astype(BF16)
        need(2, 3)
        a = dot_nn(u, w[2][...]).astype(BF16)
        a_ref[...] = a
        gate = gelu(a.astype(F32)).astype(BF16)
        dz = dot_nt(c_ref[...], w[3][...])
        dz_ref[...] = dz
        store_rows(row_ref, gate.astype(F32) * dz)

    vec = (shape_of((tokens, d), BF16), 1)
    return token_kernel(body, tile, tokens, [(x, 1), (m, 1), (g, 1), (d_out, 1)],
                        [(w_up, layer), (w_down, layer), (w_gate, 1), (w_proj, 1), (w_proj, 0)],
                        [vec, (shape_of((tokens, ff), BF16), 1), vec, vec, (shape_of((tokens, d), F32), 1),
                         (shape_of((tokens * d // LANES, LANES), F32), d // LANES)],
                        [pltpu.VMEM((tile, ff), BF16), pltpu.VMEM((tokens, d), BF16)] + unpack_scratch(rows[1], heads), 76,
                        unpack_ins(rows), (), lambda ins, outs, rest, then: unpack(ins, rest[1], rest[2:], then))


def last_up(x, w_up, layer, tile=WIDE_TILE):
    tokens, ff = x.shape[0], w_up.shape[2]

    def body(need, ins, w, outs, rest):
        need()
        up, = w
        x_f = ins[0][...].astype(F32)
        u = (x_f * rms(x_f)).astype(BF16)
        mlp_up(u, up, None, outs[0])

    return token_kernel(body, tile, tokens, [(x, 1)], [(w_up, layer)],
                        [(shape_of((tokens, ff), BF16), 1)], [], 22)[0]


def last_down(x, h, a, e, w_down, w_proj, layer, which, tile=TILE):
    tokens, d = x.shape
    ff = h.shape[1]

    def body(need, ins, w, outs, rest):
        x_ref, h_ref, a_ref, e_ref = ins
        act = rest[0]
        need()
        down, proj = w
        gate = gelu(a_ref[...].astype(F32)).astype(BF16)
        z = (gate.astype(F32) * e_ref[...].astype(F32)).astype(BF16)
        for j in range(ff // CHUNK):
            cols = slice(j * CHUNK, (j + 1) * CHUNK)
            act[:, cols] = gelu(h_ref[:, cols].astype(F32)).astype(BF16)
        for n in range(d // COLS):
            cols = slice(n * COLS, (n + 1) * COLS)
            m = dot_nn(act[...], down[:, cols]).astype(BF16)
            q = dot_nn(z, proj[:, cols]).astype(BF16)
            outs[0][:, cols] = ((x_ref[:, cols].astype(F32) + m.astype(F32)) + q.astype(F32)).astype(BF16)

    return token_kernel(body, tile, tokens, [(x, 1), (h, 1), (a, 1), (e, 1)],
                        [(w_down, layer), (w_proj, which)], [(shape_of(x.shape, BF16), 1)],
                        [pltpu.VMEM((tile, ff), BF16)], 30)[0]


def back_mlp(c_b, h_ref, w_up, w_down, dh):
    chunk = CHUNK
    for j in range(h_ref.shape[1] // chunk):
        cols = slice(j * chunk, (j + 1) * chunk)
        d_act = dot_nt(c_b, w_down[cols, :])
        dh[:, cols] = gelu_bwd(h_ref[:, cols].astype(F32), d_act).astype(BF16)
    return jnp.concatenate([dot_nt(dh[...], w_up[n * COLS:(n + 1) * COLS, :]) for n in range(w_up.shape[0] // COLS)], axis=1)


def back_norm(c_f, x_ref, du):
    x_f = x_ref[...].astype(F32)
    s = rms(x_f)
    return c_f + (s * du - x_f * (s * s * s) * jnp.mean(x_f * du, axis=-1, keepdims=True))


def back_table(c, h, x, a, dz, rows, w_up, w_down, w_gate, layer, which, heads, tile=TILE):
    tokens, d = x.shape
    ff = h.shape[1]
    unpack = unpack_step(*rows[:3], heads)

    def first_step(ins, outs, rest, then):
        unpack(ins, rest[2], rest[4:], then)
        done = pltpu.make_async_copy(rest[2], outs[0], rest[3])
        done.start()
        done.wait()

    def body(need, ins, w, outs, rest):
        c_ref, h_ref, x_ref, a_ref, dz_ref = ins
        need()
        up, down, w_g = w
        e = tile_of(rest[2], tile)[...].astype(F32)
        d_gate = gelu_bwd(a_ref[...].astype(F32), dz_ref[...] * e).astype(BF16)
        rest[1][...] = dot_nt(d_gate, w_g[...])
        du = back_mlp(c_ref[...], h_ref, up, down, rest[0]) + rest[1][...]
        outs[0][...] = back_norm(c_ref[...].astype(F32), x_ref, du)

    return token_kernel(body, tile, tokens,
                        [(c, 1), (h, 1), (x, 1), (a, 1), (dz, 1)],
                        [(w_up, layer), (w_down, layer), (w_gate, which)],
                        [(shape_of((tokens, d), F32), 1)],
                        [pltpu.VMEM((tile, ff), BF16), pltpu.VMEM((tile, d), F32), pltpu.VMEM((tokens, d), BF16),
                         pltpu.SemaphoreType.DMA] + unpack_scratch(rows[1], heads), 72,
                        unpack_ins(rows), [shape_of((tokens, d), BF16)], first_step)


def back_plain(c, h, x, g, w_up, w_down, w_proj, layer, which, tile=TILE):
    tokens, d = x.shape
    ff = h.shape[1]

    def body(need, ins, w, outs, rest):
        c_ref, h_ref, x_ref, g_ref = ins
        need()
        up, down, proj = w
        du = back_mlp(c_ref[...].astype(BF16), h_ref, up, down, rest[0])
        c_low = back_norm(c_ref[...], x_ref, du).astype(BF16)
        store_rows(rest[-1], g_ref[...].astype(F32) * dot_nt(c_low, proj[...]))

    return token_kernel(body, tile, tokens, [(c, 1), (h, 1), (x, 1), (g, 1)],
                        [(w_up, layer), (w_down, layer), (w_proj, which)], [],
                        [pltpu.VMEM((tile, ff), BF16)], 58,
                        mirror=(shape_of((tokens * d // LANES, LANES), F32), d // LANES, 11))


def split_rows(tables, place):
    n_tab, rows, width = tables.shape
    blk = rows // PLANE

    def kernel(place_ref, src, out, buf, isem, osem):
        reads = [pltpu.make_async_copy(src.at[t], buf.at[t], isem.at[t]) for t in range(n_tab)]
        for c in reads:
            c.start()
        writes = []
        for t in range(n_tab):
            reads[t].wait()
            for b in range(PLANE):
                writes.append(pltpu.make_async_copy(buf.at[t, pl.ds(b * blk, blk)], out.at[place_ref[0] ^ b, t], osem.at[t * PLANE + b]))
                writes[-1].start()
        for c in writes:
            c.wait()

    return pl.pallas_call(
        kernel, out_shape=shape_of((PLANE, n_tab, blk, width), tables.dtype), in_specs=[SMEM_SPEC, ANY_SPEC], out_specs=ANY_SPEC,
        scratch_shapes=[pltpu.VMEM(tables.shape, tables.dtype), pltpu.SemaphoreType.DMA((n_tab,)),
                        pltpu.SemaphoreType.DMA((n_tab * PLANE,))],
        compiler_params=local_params(), name="split_rows", cost_estimate=cost(4))(place, tables)


def make_ids(distinct, start, count, peak, rnd, rows):
    n_tab, n_row = distinct.shape[:2]
    n_tgt = count.shape[0] // n_tab
    depth, per = -(-SLOTS // LANES), IDW // LANES

    def kernel(name_ref, start_ref, count_ref, peak_ref, rnd_ref, out_ref):
        lane = lax.broadcasted_iota(jnp.int32, (1, LANES), 1)
        shift = rnd_ref[0] * SLOTS
        for t in range(n_tab):
            out_ref[:, t * per:(t + 1) * per, :] = jnp.full((n_tgt, per, LANES), peak_ref[t], jnp.int32)
            for g in range(n_tgt):
                left = jnp.clip(count_ref[t * n_tgt + g] - shift, 0, SLOTS)
                at = start_ref[t * n_tgt + g] + shift
                row, off = at // LANES, lax.rem(at, LANES)
                turned = [pltpu.roll(name_ref[t, jnp.minimum(row + i, n_row - 1)], lax.rem(LANES - off, LANES), axis=1)
                          for i in range(depth + 1)]
                for i in range(depth):
                    ids = 2 * (jnp.where(lane < LANES - off, turned[i], turned[i + 1]) & (rows - 1))
                    out_ref[g, t * per + i:t * per + i + 1, :] = jnp.where(i * LANES + lane < left, ids, 2 * rows)

    return pl.pallas_call(
        kernel, out_shape=shape_of((n_tgt, n_tab * per, LANES), jnp.int32),
        in_specs=[VMEM_SPEC] + [SMEM_SPEC] * 4, out_specs=VMEM_SPEC, compiler_params=local_params(), name="make_ids",
        cost_estimate=cost(3),
    )(distinct, start, count, peak, jnp.reshape(rnd, (1,)).astype(jnp.int32))


def unpack_rows(idx, rec_own, rec_pair, heads):
    step = unpack_step(idx, rec_own, rec_pair, heads)

    def kernel(idx_ref, own_ref, pair_ref, out_ref, *scratch):
        step((idx_ref, own_ref, pair_ref), out_ref, scratch, lambda: None)

    return pl.pallas_call(
        kernel, out_shape=unpacked(idx, rec_own, heads), in_specs=[SMEM_SPEC, ANY_SPEC, ANY_SPEC], out_specs=VMEM_SPEC,
        scratch_shapes=unpack_scratch(rec_own, heads), compiler_params=local_params(), name="unpack_rows", cost_estimate=cost(16),
    )(idx, rec_own, rec_pair)


def pack_rows(pos, dst, span, grad_own, grad_pair, n_tgt):
    n = grad_own.shape[0]
    n_row = 2 * n_tgt * SLOTS
    low = I32.max

    def kernel(pos_ref, dst_ref, span_ref, own_ref, pair_ref, out_ref, g_ref, stage, sem):
        first = pltpu.make_async_copy(own_ref, g_ref.at[pl.ds(0, n)], sem.at[0])
        second = pltpu.make_async_copy(pair_ref, g_ref.at[pl.ds(n, n)], sem.at[1])
        first.start()
        second.start()
        first.wait()
        second.wait()

        begin, size = span_ref[0], span_ref[1]

        def blk(b, acc):
            base = begin + b * UNROLL
            for j in range(UNROLL):
                p = pos_ref[base + j]
                row = g_ref[pair_at(p & low), :]
                acc = row + jnp.where(jnp.full((2, LANES), p, jnp.int32) < 0, acc, 0.0)
                stage[pair_at(dst_ref[base + j]), :] = acc
            return acc

        lax.fori_loop(0, (size + UNROLL - 1) // UNROLL, blk, jnp.zeros((2, LANES), F32))
        done = pltpu.make_async_copy(stage.at[pl.ds(0, n_row)], out_ref, sem.at[0])
        done.start()
        done.wait()

    return pl.pallas_call(
        kernel, out_shape=shape_of((n_row, LANES), F32),
        in_specs=[SMEM_SPEC, SMEM_SPEC, SMEM_SPEC, ANY_SPEC, ANY_SPEC], out_specs=ANY_SPEC,
        scratch_shapes=[pltpu.VMEM((2 * n, LANES), F32), pltpu.VMEM((n_row + 8, LANES), F32), pltpu.SemaphoreType.DMA((2,))],
        compiler_params=local_params(), name="pack_rows", cost_estimate=cost(26),
    )(pos, dst, span, grad_own, grad_pair)


def owner_scatter(ids, rec, rows, place):
    n_src = rec.shape[0] // (2 * SLOTS)
    per = UNROLL

    blk_rows = 2 * rows // PLANE

    def kernel(ids_ref, place_ref, rec_ref, *refs):
        outs, (acc, buf, sem, osem) = refs[:PLANE], refs[PLANE:]
        reads = [pltpu.make_async_copy(rec_ref.at[pl.ds(s * 2 * SLOTS, 2 * SLOTS)], buf.at[pl.ds(s * 2 * SLOTS, 2 * SLOTS)], sem.at[s])
                 for s in range(n_src)]
        for c in reads:
            c.start()

        def zero(i, c):
            acc[pl.ds(i * LANES, LANES), :] = jnp.zeros((LANES, LANES), F32)
            return c

        lax.fori_loop(0, 2 * rows // LANES, zero, 0)
        for s in range(n_src):
            reads[s].wait()

            def blk(b, c):
                at = [pair_at(ids_ref[s * IDW + b * per + j]) for j in range(per)]
                base = pl.multiple_of((s * SLOTS + b * per) * 2, 2 * per)
                new = [acc[i, :] + buf[pl.ds(base + 2 * j, 2), :] for j, i in enumerate(at)]
                for i, v in zip(at, new):
                    acc[i, :] = v
                return c

            lax.fori_loop(0, SLOTS // per, blk, 0)
        writes = []
        for b in range(PLANE):
            at = pl.multiple_of((place_ref[0] ^ b) * blk_rows, blk_rows)
            writes.append(pltpu.make_async_copy(acc.at[pl.ds(at, blk_rows)], outs[b], osem.at[b]))
            writes[-1].start()
        for c in writes:
            c.wait()

    return pl.pallas_call(
        kernel, out_shape=[shape_of((blk_rows, LANES), F32)] * PLANE, in_specs=[SMEM_SPEC, SMEM_SPEC, ANY_SPEC],
        out_specs=[ANY_SPEC] * PLANE,
        scratch_shapes=[pltpu.VMEM((2 * rows + 8, LANES), F32), pltpu.VMEM((n_src * 2 * SLOTS, LANES), F32),
                        pltpu.SemaphoreType.DMA((n_src,)), pltpu.SemaphoreType.DMA((PLANE,))],
        compiler_params=local_params(), name="owner_scatter", cost_estimate=cost(20),
    )(ids, place, rec)


def finish_table(blocks, grads, which, n_tab):
    blk_rows = blocks[0].shape[0]
    blk = blk_rows // 2
    shape = (n_tab, PLANE * blk, COLS)
    first = grads is None

    def kernel(*refs):
        out, buf, stage, isem, osem = refs[-5:]
        reads = [pltpu.make_async_copy(refs[b], buf.at[b], isem.at[b]) for b in range(PLANE)]
        for c in reads:
            c.start()
        writes = []
        for b in range(PLANE):
            reads[b].wait()
            for c in range(2):
                stage[b, :, c * LANES:(c + 1) * LANES] = buf[b, pl.ds(c, blk, stride=2), :]
            writes.append(pltpu.make_async_copy(stage.at[b], out.at[which, pl.ds(b * blk, blk)], osem.at[b]))
            writes[-1].start()
        for c in writes:
            c.wait()

    args = list(blocks) + ([] if first else [grads])
    return pl.pallas_call(
        kernel, out_shape=shape_of(shape, F32), in_specs=[ANY_SPEC] * len(args), out_specs=ANY_SPEC,
        scratch_shapes=[pltpu.VMEM((PLANE, blk_rows, LANES), F32), pltpu.VMEM((PLANE, blk, COLS), F32),
                        pltpu.SemaphoreType.DMA((PLANE,)), pltpu.SemaphoreType.DMA((PLANE,))],
        input_output_aliases={} if first else {PLANE: 0},
        compiler_params=local_params(), name="finish_table", cost_estimate=cost(8))(*args)


def swap_cores(x, n_dev):
    return lax.ppermute(x, 'emb', [(i, i ^ 1) for i in range(n_dev)])


def chip_trade(x, n_dev):
    groups = [list(range(c, n_dev, 2)) for c in range(2)]
    return lax.all_to_all(x, 'emb', 0, 0, axis_index_groups=groups, tiled=True)


def chip_exchange(blocks, cid, n_chip):
    def kernel(x_ref, o_ref, ssem, rsem, lsem):
        me = lax.axis_index('emb')
        chip = me // 2
        barrier = pltpu.get_barrier_semaphore()
        for d in range(1, n_chip):
            pl.semaphore_signal(barrier, inc=1, device_id=(me ^ (2 * d),), device_id_type=MESH)
        pl.semaphore_wait(barrier, n_chip - 1)
        copies = [pltpu.make_async_copy(x_ref.at[chip], o_ref.at[chip], lsem)]
        for d in range(1, n_chip):
            copies.append(pltpu.make_async_remote_copy(
                src_ref=x_ref.at[chip ^ d], dst_ref=o_ref.at[chip], send_sem=ssem.at[d], recv_sem=rsem.at[d],
                device_id=(me ^ (2 * d),), device_id_type=MESH))
        for c in copies:
            c.start()
        for c in copies:
            c.wait()

    return pl.pallas_call(
        kernel, out_shape=shape_of(blocks.shape, blocks.dtype), in_specs=[ANY_SPEC], out_specs=ANY_SPEC,
        scratch_shapes=[pltpu.SemaphoreType.DMA((n_chip,)), pltpu.SemaphoreType.DMA((n_chip,)), pltpu.SemaphoreType.DMA],
        compiler_params=remote_params(cid), name="chip_exchange", cost_estimate=cost(100))(blocks)


def plane_trade(x, n_dev):
    groups = [list(range(z, z + PLANE)) for z in range(0, n_dev, PLANE)]
    return lax.all_to_all(x, 'emb', 0, 0, axis_index_groups=groups, tiled=True)


def empty_array(shape, dtype):
    return pl.pallas_call(lambda o: None, out_shape=shape_of(shape, dtype), out_specs=ANY_SPEC, name="empty")()


def place_trade(blocks, n_dev):
    return [blocks[0]] + [lax.ppermute(blocks[b], 'emb', [(i, i ^ b) for i in range(n_dev)]) for b in range(1, PLANE)]


def after(x, *deps):
    return lax.optimization_barrier((x,) + deps)[0]


def sort_requests(ids_pair, rows_dev, n_dev):
    n = ids_pair.shape[0]
    n_chip = n_dev // 2
    blk = rows_dev // PLANE
    owner, local = ids_pair // rows_dev, lax.rem(ids_pair, rows_dev)
    server = owner ^ (local // blk)
    name = (lax.rem(server, 2) * n_chip + server // 2) * rows_dev + lax.rem(owner, PLANE) * blk + lax.rem(local, blk)
    return lax.sort(name * n + jnp.arange(n, dtype=jnp.int32))


def route_plan(key, n_own, rows_dev, n_dev, me):
    n = key.shape[0]
    n_chip = n_dev // 2
    sid, pos = key // n, lax.rem(key, n)
    n_low = jnp.sum((sid < n_chip * rows_dev).astype(jnp.int32))
    first = sid != jnp.concatenate([jnp.full((1,), -1, jnp.int32), sid[:-1]])
    slot = jnp.cumsum(first.astype(jnp.int32)) - 1
    tgt = sid // rows_dev
    bound = jnp.arange(n_dev + 1, dtype=jnp.int32)
    start = jnp.sum((first[None, :] & (tgt[None, :] < bound[:, None])).astype(jnp.int32), axis=1)
    rank = slot - jnp.sum(jnp.where(tgt[None, :] == bound[:-1, None], start[:-1, None], 0), axis=0)
    code = tgt * (2 * rows_dev) + rank
    count = start[1:] - start[:-1]
    core = lax.rem(me, 2)
    size = jnp.where(core == 0, n_low, n - n_low)
    begin = jnp.where(core == 0, 0, n_low)
    mine = sid // (n_chip * rows_dev) == core
    start = lax.dynamic_slice(start, (core * n_chip,), (n_chip,))
    return dict(pos=jnp.pad(2 * pos + jnp.where(first, 0, I32.min), (0, UNROLL)),
                code=jnp.pad(jnp.where(mine, code, -1), (0, UNROLL), constant_values=-1),
                span=jnp.stack([begin, size]), distinct=jnp.where(first & mine, sid, I32.max), start=start - start[0],
                by_pos=jnp.where(pos < n_own, pos * (n_dev * 2 * rows_dev) + code, I32.max),
                count=lax.dynamic_slice(count, (core * n_chip,), (n_chip,)), peak=jnp.max(count))


def round_slot(code, span, rnd, trash, width):
    tgt, rank = code // span, lax.rem(code, span) - rnd * SLOTS
    inside = (code >= 0) & (rank >= 0) & (rank < SLOTS)
    return jnp.where(inside, tgt * width + rank, trash)


def solution(mesh):
    n_dev = mesh.shape['emb']
    n_chip = n_dev // 2
    tok_spec = P('emb', None)
    tab_spec = P(None, 'emb', None)

    def step(x_start, d_out, token_ids, w_up, w_down, w_gate, w_proj, tables):
        n_tab, n_tok, n_heads = token_ids.shape
        rows_dev, row_width = tables.shape[1], tables.shape[2]
        n_req = n_tok * n_heads
        tail = (row_width // LANES, LANES)
        me = lax.axis_index('emb')
        core = lax.rem(me, 2)

        flat_ids = token_ids.reshape(n_tab, n_req)
        ids_pair = jnp.concatenate([flat_ids, swap_cores(flat_ids, n_dev)], axis=1)
        place = lax.rem(me, PLANE).reshape(1)
        split = split_rows(tables, place)
        served = plane_trade(split, n_dev)
        keys = [sort_requests(after(ids_pair, split)[t], rows_dev, n_dev) for t in range(n_tab)]

        plans = [route_plan(keys[t], n_req, rows_dev, n_dev, me) for t in range(n_tab)]
        distinct = lax.sort(jnp.stack([plan['distinct'] for plan in plans]), dimension=1)
        x1 = layer_plain(after(x_start, *[plan['distinct'] for plan in plans]), w_up, w_down, 0)
        distinct = distinct.reshape(n_tab, -1, 1, LANES)
        span = 2 * rows_dev
        in_order = lax.sort(after(jnp.stack([plan['by_pos'] for plan in plans]), distinct), dimension=1)
        code_own = lax.rem(in_order[:, :n_req], n_dev * span)

        def half_slot(plan, rnd, width, trash):
            code = plan['code']
            code = jnp.where(code >= 0, lax.rem(code, n_chip * span), code)
            return round_slot(code, span, rnd, trash, width)

        def id_blocks(tabs, rnd):
            start, count = (jnp.concatenate([plans[t][key] for t in tabs]) for key in ('start', 'count'))
            peak = jnp.stack([plans[t]['peak'] for t in tabs])
            return make_ids(distinct[tabs[0]:tabs[-1] + 1], start, count, peak, rnd, rows_dev)

        blocks = id_blocks(range(n_tab), jnp.int32(0))
        got = chip_exchange(after(blocks, served, x1), 9, n_chip).reshape(n_chip, n_tab, IDW)
        first_ids = [got[:, t].reshape(n_chip * IDW) for t in range(n_tab)]
        rounds = [(jnp.max(got[:, t, IDW - 1]) + SLOTS - 1) // SLOTS for t in range(n_tab)]

        def more_ids(which, rnd, cid):
            return chip_exchange(id_blocks([which], rnd), cid, n_chip).reshape(n_chip * IDW)

        def own_slot(which, rnd):
            half = n_chip * SLOTS
            slot = round_slot(code_own[which], span, rnd, 2 * half, SLOTS)
            return jnp.where((core == 0) | (slot == 2 * half), slot, lax.rem(slot + half, 2 * half))

        def unpack(which, rnd, own):
            return unpack_rows(own_slot(which, rnd), own, swap_cores(own, n_dev), n_heads)

        def late_rows(start):
            def more(state):
                rnd, now = state[0], []
                for t in range(n_tab):
                    sent = owner_gather(more_ids(t, rnd, t), served, t, n_chip).reshape((n_chip, SLOTS) + tail)
                    new = unpack(t, rnd, chip_exchange(sent, 2 + t, n_chip).reshape((n_chip * SLOTS,) + tail))
                    mine = lax.rem(code_own[t], span) // SLOTS == rnd
                    now.append(jnp.where(jnp.repeat(mine, row_width).reshape(new.shape), new, state[1 + t]))
                return (rnd + 1, *now)

            most = jnp.maximum(*rounds)
            return lax.while_loop(lambda s: s[0] < most, more, (jnp.int32(1), *start))[1:]

        def parts(which, own):
            return own_slot(which, 0), own, swap_cores(own, n_dev), late[which], rounds[which].reshape(1)

        def packed(which, rnd, grad_own, grad_pair):
            plan = plans[which]
            dst = 2 * half_slot(plan, rnd, SLOTS, n_chip * SLOTS)
            return pack_rows(plan['pos'], dst, plan['span'], grad_own, grad_pair, n_chip)

        def return_rest(which, first, pair):
            def more(state):
                rnd, total = state
                ids = more_ids(which, rnd, 4 + which)
                rec = chip_exchange(packed(which, rnd, *pair).reshape(n_chip, 2 * SLOTS, LANES), 6 + which, n_chip)
                new = owner_scatter(ids, rec.reshape(n_chip * 2 * SLOTS, LANES), rows_dev, place)
                return rnd + 1, [p + q for p, q in zip(total, new)]

            return lax.while_loop(lambda s: s[0] < rounds[which], more, (jnp.int32(1), list(first)))[1]

        sent0 = owner_gather(first_ids[0], served, 0, n_chip)
        fetched0 = chip_trade(sent0, n_dev)
        m1, g1, sent1 = layer_table_head(after(x1, sent0), w_up, w_down, w_gate, 1, 0, first_ids[1], served, n_chip)
        late = late_rows([after(empty_array((n_tok, n_heads * row_width), BF16), m1, fetched0) for _ in range(n_tab)])
        rows0 = parts(0, after(fetched0, m1))
        fetched1 = chip_trade(after(sent1, fetched0, *late), n_dev)
        x2, h2, x3, a3, dz3, rows3 = layer_middle(x1, m1, g1, rows0, d_out, w_up, w_down, w_gate, w_proj, 2, n_heads)
        pair1 = rows3, swap_cores(rows3, n_dev)
        h3 = last_up(x3, w_up, 3)
        rows1 = parts(1, after(fetched1, h3))
        sent1 = packed(1, 0, pair1[0], after(pair1[1], h3))
        returned1 = chip_trade(after(sent1, fetched1), n_dev)
        c2, e3 = back_table(after(d_out, sent1), h3, x3, a3, dz3, rows1, w_up, w_down, w_gate, 3, 1, n_heads)
        pair0 = back_plain(c2, h2, x2, g1, w_up, w_down, w_proj, 2, 0)
        sent0 = packed(0, 0, *pair0)
        returned0 = chip_trade(after(sent0, returned1), n_dev)
        total1 = owner_scatter(first_ids[1], after(returned1, sent0), rows_dev, place)
        total1 = return_rest(1, total1, pair1)
        placed1 = place_trade(total1, n_dev)
        x_end = last_down(after(x3, *total1), h3, a3, e3, w_down, w_proj, 3, 1)
        total0 = owner_scatter(first_ids[0], after(returned0, x_end), rows_dev, place)
        total0 = return_rest(0, total0, pair0)
        placed0 = place_trade(total0, n_dev)
        grads = finish_table([after(p, *total0) for p in placed1], None, 1, n_tab)
        grads = finish_table(placed0, grads, 0, n_tab)
        return x_end, grads

    return jax.shard_map(step, mesh=mesh, in_specs=(tok_spec, tok_spec, tab_spec, P(), P(), P(), P(), tab_spec),
                         out_specs=(tok_spec, tab_spec), check_vma=False)
```

```python
import jax
import jax.numpy as jnp
from jax import lax
from jax.experimental import pallas as pl
from jax.experimental.pallas import tpu as pltpu
from jax.sharding import PartitionSpec as P


EPS = 1e-6
C1 = 0.7978845608028654
C2 = C1 * 0.044715
BF16 = jnp.bfloat16
I32 = jnp.iinfo(jnp.int32)
F32 = jnp.float32
VMEM_LIMIT = 62 * 1024 * 1024
MESH = pl.DeviceIdType.MESH
PLANE = 8
SLOTS = 336
IDW = 1024
UNROLL = 16
UNPACK = 32
LANES = 128
COLS = 256
CHUNK = 512
TILE = 256
WIDE_TILE = 512

SMEM_SPEC = pl.BlockSpec(memory_space=pltpu.SMEM)
VMEM_SPEC = pl.BlockSpec(memory_space=pltpu.VMEM)
ANY_SPEC = pl.BlockSpec(memory_space=pl.ANY)


def local_params():
    return pltpu.CompilerParams(vmem_limit_bytes=VMEM_LIMIT)


def remote_params(cid):
    return pltpu.CompilerParams(vmem_limit_bytes=VMEM_LIMIT, collective_id=cid, has_side_effects=True)


def cost(us):
    return pl.CostEstimate(flops=int(us * 9e8), bytes_accessed=2**23, transcendentals=0)


def shape_of(shape, dtype):
    return jax.ShapeDtypeStruct(shape, dtype)


def gelu(x):
    half = 0.5 * x
    return half + half * jnp.tanh(x * (C1 + C2 * (x * x)))


def gelu_bwd(x, ct):
    x2 = x * x
    t = jnp.tanh(x * (C1 + C2 * x2))
    return ct * ((0.5 + 0.5 * t) + (x * (0.5 - (0.5 * t) * t)) * (C1 + (3 * C2) * x2))


def dot_nn(a, b):
    return jnp.dot(a, b, preferred_element_type=F32)


def dot_nt(a, b):
    return lax.dot_general(a, b, (((1,), (1,)), ((), ())), preferred_element_type=F32)


def rms(x_f):
    return lax.rsqrt(jnp.mean(x_f * x_f, axis=-1, keepdims=True) + EPS)


def pair_at(index):
    return pl.ds(pl.multiple_of(index, 2), 2)


def owner_gather(ids, served, which, n_src):
    work = gather_step(served, which, n_src)

    def kernel(ids_ref, served_ref, out_ref, *scratch):
        work((ids_ref, served_ref), out_ref, scratch, lambda: None)

    return pl.pallas_call(
        kernel, out_shape=gathered(served, n_src), in_specs=[SMEM_SPEC, ANY_SPEC], out_specs=VMEM_SPEC,
        scratch_shapes=gather_scratch(served), compiler_params=local_params(), name="owner_gather", cost_estimate=cost(14),
    )(ids, served)


def gathered(served, n_src):
    return shape_of((n_src * SLOTS, served.shape[3] // LANES, LANES), BF16)


def gather_scratch(served):
    blk, width = served.shape[2:]
    return [pltpu.VMEM((PLANE, blk, width), BF16), pltpu.VMEM((PLANE * blk * width // LANES + 8, LANES), F32),
            pltpu.SemaphoreType.DMA((PLANE,))]


def gather_step(served, which, n_src):
    blk, width = served.shape[2:]
    pieces = width // LANES

    def work(ins, out_ref, scratch, then):
        ids_ref, served_ref = ins
        native, flat, isem = scratch
        reads = [pltpu.make_async_copy(served_ref.at[b, which], native.at[b], isem.at[b]) for b in range(PLANE)]
        for c in reads:
            c.start()
        for b in range(PLANE):
            reads[b].wait()
            for c in range(pieces):
                flat[pl.ds(b * blk * pieces + c, blk, stride=pieces), :] = native[b, :, c * LANES:(c + 1) * LANES].astype(F32)
        then()

        def src(s, c):
            def part(b, c):
                for j in range(UNROLL):
                    r = b * UNROLL + j
                    out_ref[s * SLOTS + r] = flat[pair_at(ids_ref[s * IDW + r]), :].astype(BF16)
                return c

            lax.fori_loop(0, SLOTS // UNROLL, part, 0)
            return c

        lax.fori_loop(0, n_src, src, 0)

    return work


def unpacked(idx, rec, heads):
    return shape_of((idx.shape[0] // heads, heads * rec.shape[1] * LANES), BF16)


def unpack_scratch(rec, heads):
    half, pieces = rec.shape[0], rec.shape[1]
    rows = pltpu.VMEM((TILE * heads * pieces, LANES), F32)
    return [pltpu.VMEM((2 * half + 8, pieces, LANES), BF16), rows, pltpu.SemaphoreType.DMA((2,)), rows,
            pltpu.VMEM((TILE, heads * pieces * LANES), BF16)]


def unpack_step(idx, rec_own, rec_pair, heads):
    n = idx.shape[0]
    half, pieces = rec_own.shape[0], rec_own.shape[1]
    per = heads * pieces

    def work(ins, out_ref, scratch, then):
        idx_ref, own_ref, pair_ref = ins[:3]
        rec, stage, sem, more, native = scratch
        copies = [pltpu.make_async_copy(own_ref, rec.at[pl.ds(0, half)], sem.at[0]),
                  pltpu.make_async_copy(pair_ref, rec.at[pl.ds(half, half)], sem.at[1])]
        for c in copies:
            c.start()
        for c in copies:
            c.wait()
        then()

        def part(i, c):
            first = i * (TILE * heads)

            def blk(b, c):
                for j in range(UNPACK):
                    row = rec[idx_ref[first + b * UNPACK + j]]
                    stage[pl.ds(pl.multiple_of(b * UNPACK * pieces, UNPACK * pieces) + pieces * j, pieces), :] = row.astype(F32)
                return c

            lax.fori_loop(0, TILE * heads // UNPACK, blk, 0)
            if len(ins) > 3:
                late_ref, rounds_ref = ins[3:]

                @pl.when(rounds_ref[0] > 1)
                def _():
                    fetch = pltpu.make_async_copy(late_ref.at[pl.ds(i * TILE, TILE)], native, sem.at[0])
                    fetch.start()
                    fetch.wait()
                    store_rows(more, native[...].astype(F32))

                    def patch(r, c):
                        @pl.when(idx_ref[first + r] == 2 * half)
                        def _():
                            stage[pair_at(2 * r), :] = more[pair_at(2 * r), :]

                        return c

                    lax.fori_loop(0, TILE * heads, patch, 0)
            for c in range(per):
                out_ref[pl.ds(i * TILE, TILE), c * LANES:(c + 1) * LANES] = stage[pl.ds(c, TILE, stride=per), :].astype(BF16)
            return c

        lax.fori_loop(0, n // heads // TILE, part, 0)

    return work


def token_kernel(body, tile, tokens, ins, weights, outs, scratch, us, extra_ins=(), extra_outs=(), first_step=None, mirror=None):
    steps = tokens // tile
    if mirror is not None:
        extra_outs = list(extra_outs) + [mirror[0]] * 2
        scratch = list(scratch) + [pltpu.VMEM((2, tile * mirror[1]) + mirror[0].shape[1:], mirror[0].dtype)] + [
            pltpu.SemaphoreType.DMA((steps,))] * 3
    ins = list(ins) + [(a, spec) for a, spec in extra_ins]
    outs = list(outs) + [(s, ANY_SPEC) for s in extra_outs]
    n_in, n_w, n_out = len(ins), len(weights), len(outs)
    n_own_in, n_own_out = n_in - len(extra_ins), n_out - len(extra_outs)

    def kernel(*refs):
        in_refs = refs[:n_in]
        w_hbm = refs[n_in:n_in + n_w]
        out_refs = refs[n_in + n_w:n_in + n_w + n_out]
        w_vmem = refs[n_in + n_w + n_out:n_in + 2 * n_w + n_out]
        sem = refs[n_in + 2 * n_w + n_out]
        rest = refs[n_in + 2 * n_w + n_out + 1:]
        copies = [pltpu.make_async_copy(w_hbm[i].at[weights[i][1]], w_vmem[i], sem.at[i]) for i in range(n_w)]
        opening = pl.program_id(0) == 0

        @pl.when(opening)
        def _():
            def start_weights():
                for c in copies:
                    c.start()

            if first_step is None:
                start_weights()
            else:
                first_step(in_refs[n_own_in:], out_refs[n_own_out:], rest, start_weights)

        def need(*which):
            @pl.when(opening)
            def _():
                for i in which or range(n_w):
                    copies[i].wait()

        if mirror is None:
            body(need, in_refs[:n_own_in], w_vmem, out_refs[:n_own_out], rest)
            return
        i = pl.program_id(0)
        other = lax.axis_index('emb') ^ 1
        barrier = pltpu.get_barrier_semaphore()
        own, pair = out_refs[-2:]
        stage, keep_sem, send_sem, recv_sem = rest[-4:]
        per = tile * mirror[1]

        def keep(j):
            return pltpu.make_async_copy(stage.at[lax.rem(j, 2)], own.at[pl.ds(j * per, per)], keep_sem.at[j])

        def send(j):
            return pltpu.make_async_remote_copy(
                src_ref=own.at[pl.ds(j * per, per)], dst_ref=pair.at[pl.ds(j * per, per)], send_sem=send_sem.at[j],
                recv_sem=recv_sem.at[j], device_id=(other,), device_id_type=MESH)

        @pl.when(opening)
        def _():
            pl.semaphore_signal(barrier, inc=1, device_id=(other,), device_id_type=MESH)
            pl.semaphore_wait(barrier, 1)

        body(need, in_refs[:n_own_in], w_vmem, out_refs[:n_own_out], list(rest[:-4]) + [stage.at[lax.rem(i, 2)]])
        keep(i).start()

        @pl.when(i > 0)
        def _():
            keep(i - 1).wait()
            send(i - 1).start()

        @pl.when(i == steps - 1)
        def _():
            keep(i).wait()
            send(i).start()
            for j in range(steps):
                send(j).wait()

    def tiled(shape, per):
        if isinstance(per, pl.BlockSpec):
            return per
        return pl.BlockSpec((tile * per,) + shape[1:], lambda i: (i,) + (0,) * (len(shape) - 1))

    in_specs = [tiled(a.shape, per) for a, per in ins] + [ANY_SPEC] * n_w
    out_specs = [tiled(s.shape, per) for s, per in outs]
    w_scratch = [pltpu.VMEM(w.shape[1:], w.dtype) for w, _ in weights]
    return pl.pallas_call(
        kernel, grid=(tokens // tile,), out_shape=[s for s, _ in outs], in_specs=in_specs, out_specs=out_specs,
        scratch_shapes=w_scratch + [pltpu.SemaphoreType.DMA((n_w,))] + list(scratch),
        compiler_params=local_params() if mirror is None else remote_params(mirror[2]), cost_estimate=cost(us),
    )(*[a for a, _ in ins], *[w for w, _ in weights])


def mlp_up(u, w_up, act, h_ref, chunk=CHUNK):
    for j in range(w_up.shape[1] // chunk):
        cols = slice(j * chunk, (j + 1) * chunk)
        h = dot_nn(u, w_up[:, cols]).astype(BF16)
        if h_ref is not None:
            h_ref[:, cols] = h
        if act is not None:
            act[:, cols] = gelu(h.astype(F32)).astype(BF16)


def store_rows(ref, value):
    tokens, width = value.shape
    n = width // LANES
    for c in range(n):
        ref[pl.ds(c, tokens, stride=n), :] = value[:, c * LANES:(c + 1) * LANES]


def tile_of(ref, tile):
    return ref.at[pl.ds(pl.multiple_of(pl.program_id(0) * tile, tile), tile), :]


def unpack_ins(rows):
    return list(zip(rows, [SMEM_SPEC, ANY_SPEC, ANY_SPEC, ANY_SPEC, SMEM_SPEC]))


def layer_plain(x, w_up, w_down, layer, tile=WIDE_TILE):
    tokens, d = x.shape

    def body(need, ins, w, outs, rest):
        need()
        up, down = w
        x_f = ins[0][...].astype(F32)
        u = (x_f * rms(x_f)).astype(BF16)
        mlp_up(u, up, rest[0], None)
        for q in range(d // COLS):
            cols = slice(q * COLS, (q + 1) * COLS)
            m = dot_nn(rest[0][...], down[:, cols]).astype(BF16)
            outs[0][:, cols] = (ins[0][:, cols].astype(F32) + m.astype(F32)).astype(BF16)

    return token_kernel(body, tile, tokens, [(x, 1)], [(w_up, layer), (w_down, layer)],
                        [(shape_of(x.shape, BF16), 1)], [pltpu.VMEM((tile, w_up.shape[2]), BF16)], 44)[0]


def layer_table_head(x, w_up, w_down, w_gate, layer, which, ids, served, n_src, tile=WIDE_TILE):
    tokens, d = x.shape
    gather = gather_step(served, 1, n_src)
    sent = gathered(served, n_src)

    def first_step(ins, outs, rest, then):
        stage, sem = rest[-2:]
        gather(ins, stage, rest[1:-2], then)
        done = pltpu.make_async_copy(stage, outs[0], sem)
        done.start()
        done.wait()

    def body(need, ins, w, outs, rest):
        need()
        up, down, gate = w
        x_f = ins[0][...].astype(F32)
        u = (x_f * rms(x_f)).astype(BF16)
        mlp_up(u, up, rest[0], None)
        a = dot_nn(u, gate[...]).astype(BF16)
        outs[1][...] = gelu(a.astype(F32)).astype(BF16)
        for q in range(d // COLS):
            cols = slice(q * COLS, (q + 1) * COLS)
            outs[0][:, cols] = dot_nn(rest[0][...], down[:, cols]).astype(BF16)

    return token_kernel(body, tile, tokens, [(x, 1)],
                        [(w_up, layer), (w_down, layer), (w_gate, which)],
                        [(shape_of(x.shape, BF16), 1), (shape_of(x.shape, BF16), 1)],
                        [pltpu.VMEM((tile, w_up.shape[2]), BF16)] + gather_scratch(served) +
                        [pltpu.VMEM(sent.shape, BF16), pltpu.SemaphoreType.DMA], 60,
                        [(ids, SMEM_SPEC), (served, ANY_SPEC)], [sent], first_step)


def layer_middle(x, m, g, rows, d_out, w_up, w_down, w_gate, w_proj, layer, heads, tile=TILE):
    tokens, d = x.shape
    ff = w_up.shape[2]
    unpack = unpack_step(*rows[:3], heads)

    def body(need, ins, w, outs, rest):
        x_ref, m_ref, g_ref, c_ref = ins
        x2_ref, h_ref, x3_ref, a_ref, dz_ref, row_ref = outs
        act, e = rest[:2]
        need(4, 0)
        z = (g_ref[...].astype(F32) * tile_of(e, tile)[...].astype(F32)).astype(BF16)
        q = dot_nn(z, w[4][...]).astype(BF16)
        x2 = ((x_ref[...].astype(F32) + m_ref[...].astype(F32)) + q.astype(F32)).astype(BF16)
        x2_ref[...] = x2
        x_f = x2.astype(F32)
        u = (x_f * rms(x_f)).astype(BF16)
        need(1)
        mlp_up(u, w[0], act, h_ref)
        for n in range(d // COLS):
            cols = slice(n * COLS, (n + 1) * COLS)
            mm = dot_nn(act[...], w[1][:, cols]).astype(BF16)
            x3_ref[:, cols] = (x2_ref[:, cols].astype(F32) + mm.astype(F32)).astype(BF16)
        x_f = x3_ref[...].astype(F32)
        u = (x_f * rms(x_f)).astype(BF16)
        need(2, 3)
        a = dot_nn(u, w[2][...]).astype(BF16)
        a_ref[...] = a
        gate = gelu(a.astype(F32)).astype(BF16)
        dz = dot_nt(c_ref[...], w[3][...])
        dz_ref[...] = dz
        store_rows(row_ref, gate.astype(F32) * dz)

    vec = (shape_of((tokens, d), BF16), 1)
    return token_kernel(body, tile, tokens, [(x, 1), (m, 1), (g, 1), (d_out, 1)],
                        [(w_up, layer), (w_down, layer), (w_gate, 1), (w_proj, 1), (w_proj, 0)],
                        [vec, (shape_of((tokens, ff), BF16), 1), vec, vec, (shape_of((tokens, d), F32), 1),
                         (shape_of((tokens * d // LANES, LANES), F32), d // LANES)],
                        [pltpu.VMEM((tile, ff), BF16), pltpu.VMEM((tokens, d), BF16)] + unpack_scratch(rows[1], heads), 76,
                        unpack_ins(rows), (), lambda ins, outs, rest, then: unpack(ins, rest[1], rest[2:], then))


def last_up(x, w_up, layer, tile=WIDE_TILE):
    tokens, ff = x.shape[0], w_up.shape[2]

    def body(need, ins, w, outs, rest):
        need()
        up, = w
        x_f = ins[0][...].astype(F32)
        u = (x_f * rms(x_f)).astype(BF16)
        mlp_up(u, up, None, outs[0])

    return token_kernel(body, tile, tokens, [(x, 1)], [(w_up, layer)],
                        [(shape_of((tokens, ff), BF16), 1)], [], 22)[0]


def last_down(x, h, a, e, w_down, w_proj, layer, which, tile=TILE):
    tokens, d = x.shape
    ff = h.shape[1]

    def body(need, ins, w, outs, rest):
        x_ref, h_ref, a_ref, e_ref = ins
        act = rest[0]
        need()
        down, proj = w
        gate = gelu(a_ref[...].astype(F32)).astype(BF16)
        z = (gate.astype(F32) * e_ref[...].astype(F32)).astype(BF16)
        for j in range(ff // CHUNK):
            cols = slice(j * CHUNK, (j + 1) * CHUNK)
            act[:, cols] = gelu(h_ref[:, cols].astype(F32)).astype(BF16)
        for n in range(d // COLS):
            cols = slice(n * COLS, (n + 1) * COLS)
            m = dot_nn(act[...], down[:, cols]).astype(BF16)
            q = dot_nn(z, proj[:, cols]).astype(BF16)
            outs[0][:, cols] = ((x_ref[:, cols].astype(F32) + m.astype(F32)) + q.astype(F32)).astype(BF16)

    return token_kernel(body, tile, tokens, [(x, 1), (h, 1), (a, 1), (e, 1)],
                        [(w_down, layer), (w_proj, which)], [(shape_of(x.shape, BF16), 1)],
                        [pltpu.VMEM((tile, ff), BF16)], 30)[0]


def back_mlp(c_b, h_ref, w_up, w_down, dh):
    chunk = CHUNK
    for j in range(h_ref.shape[1] // chunk):
        cols = slice(j * chunk, (j + 1) * chunk)
        d_act = dot_nt(c_b, w_down[cols, :])
        dh[:, cols] = gelu_bwd(h_ref[:, cols].astype(F32), d_act).astype(BF16)
    return jnp.concatenate([dot_nt(dh[...], w_up[n * COLS:(n + 1) * COLS, :]) for n in range(w_up.shape[0] // COLS)], axis=1)


def back_norm(c_f, x_ref, du):
    x_f = x_ref[...].astype(F32)
    s = rms(x_f)
    return c_f + (s * du - x_f * (s * s * s) * jnp.mean(x_f * du, axis=-1, keepdims=True))


def back_table(c, h, x, a, dz, rows, w_up, w_down, w_gate, layer, which, heads, tile=TILE):
    tokens, d = x.shape
    ff = h.shape[1]
    unpack = unpack_step(*rows[:3], heads)

    def first_step(ins, outs, rest, then):
        unpack(ins, rest[2], rest[4:], then)
        done = pltpu.make_async_copy(rest[2], outs[0], rest[3])
        done.start()
        done.wait()

    def body(need, ins, w, outs, rest):
        c_ref, h_ref, x_ref, a_ref, dz_ref = ins
        need()
        up, down, w_g = w
        e = tile_of(rest[2], tile)[...].astype(F32)
        d_gate = gelu_bwd(a_ref[...].astype(F32), dz_ref[...] * e).astype(BF16)
        rest[1][...] = dot_nt(d_gate, w_g[...])
        du = back_mlp(c_ref[...], h_ref, up, down, rest[0]) + rest[1][...]
        outs[0][...] = back_norm(c_ref[...].astype(F32), x_ref, du)

    return token_kernel(body, tile, tokens,
                        [(c, 1), (h, 1), (x, 1), (a, 1), (dz, 1)],
                        [(w_up, layer), (w_down, layer), (w_gate, which)],
                        [(shape_of((tokens, d), F32), 1)],
                        [pltpu.VMEM((tile, ff), BF16), pltpu.VMEM((tile, d), F32), pltpu.VMEM((tokens, d), BF16),
                         pltpu.SemaphoreType.DMA] + unpack_scratch(rows[1], heads), 72,
                        unpack_ins(rows), [shape_of((tokens, d), BF16)], first_step)


def back_plain(c, h, x, g, w_up, w_down, w_proj, layer, which, tile=TILE):
    tokens, d = x.shape
    ff = h.shape[1]

    def body(need, ins, w, outs, rest):
        c_ref, h_ref, x_ref, g_ref = ins
        need()
        up, down, proj = w
        du = back_mlp(c_ref[...].astype(BF16), h_ref, up, down, rest[0])
        c_low = back_norm(c_ref[...], x_ref, du).astype(BF16)
        store_rows(rest[-1], g_ref[...].astype(F32) * dot_nt(c_low, proj[...]))

    return token_kernel(body, tile, tokens, [(c, 1), (h, 1), (x, 1), (g, 1)],
                        [(w_up, layer), (w_down, layer), (w_proj, which)], [],
                        [pltpu.VMEM((tile, ff), BF16)], 58,
                        mirror=(shape_of((tokens * d // LANES, LANES), F32), d // LANES, 11))


def split_rows(tables, place):
    n_tab, rows, width = tables.shape
    blk = rows // PLANE

    def kernel(place_ref, src, out, buf, isem, osem):
        reads = [pltpu.make_async_copy(src.at[t], buf.at[t], isem.at[t]) for t in range(n_tab)]
        for c in reads:
            c.start()
        writes = []
        for t in range(n_tab):
            reads[t].wait()
            for b in range(PLANE):
                writes.append(pltpu.make_async_copy(buf.at[t, pl.ds(b * blk, blk)], out.at[place_ref[0] ^ b, t], osem.at[t * PLANE + b]))
                writes[-1].start()
        for c in writes:
            c.wait()

    return pl.pallas_call(
        kernel, out_shape=shape_of((PLANE, n_tab, blk, width), tables.dtype), in_specs=[SMEM_SPEC, ANY_SPEC], out_specs=ANY_SPEC,
        scratch_shapes=[pltpu.VMEM(tables.shape, tables.dtype), pltpu.SemaphoreType.DMA((n_tab,)),
                        pltpu.SemaphoreType.DMA((n_tab * PLANE,))],
        compiler_params=local_params(), name="split_rows", cost_estimate=cost(4))(place, tables)


def make_ids(distinct, marks, rnd, rows):
    n_tab, n_row = distinct.shape[:2]
    n_mark = marks.shape[0] // n_tab
    n_tgt = (n_mark - 3) // 2
    depth, per = -(-SLOTS // LANES), IDW // LANES

    def kernel(name_ref, mark_ref, rnd_ref, out_ref):
        lane = lax.broadcasted_iota(jnp.int32, (1, LANES), 1)
        shift = rnd_ref[0] * SLOTS
        for t in range(n_tab):
            base = t * n_mark
            half = mark_ref[base + n_mark - 2]
            origin = mark_ref[base + half]
            out_ref[:, t * per:(t + 1) * per, :] = jnp.full((n_tgt, per, LANES), mark_ref[base + n_mark - 1], jnp.int32)
            for g in range(n_tgt):
                begin = mark_ref[base + half + g]
                left = jnp.clip(mark_ref[base + half + g + 1] - begin - shift, 0, SLOTS)
                at = begin - origin + shift
                row, off = at // LANES, lax.rem(at, LANES)
                turned = [pltpu.roll(name_ref[t, jnp.minimum(row + i, n_row - 1)], lax.rem(LANES - off, LANES), axis=1)
                          for i in range(depth + 1)]
                for i in range(depth):
                    ids = 2 * (jnp.where(lane < LANES - off, turned[i], turned[i + 1]) & (rows - 1))
                    out_ref[g, t * per + i:t * per + i + 1, :] = jnp.where(i * LANES + lane < left, ids, 2 * rows)

    return pl.pallas_call(
        kernel, out_shape=shape_of((n_tgt, n_tab * per, LANES), jnp.int32),
        in_specs=[VMEM_SPEC, SMEM_SPEC, SMEM_SPEC], out_specs=VMEM_SPEC, compiler_params=local_params(), name="make_ids",
        cost_estimate=cost(3),
    )(distinct, marks, jnp.reshape(rnd, (1,)).astype(jnp.int32))


def unpack_rows(idx, rec_own, rec_pair, heads):
    step = unpack_step(idx, rec_own, rec_pair, heads)

    def kernel(idx_ref, own_ref, pair_ref, out_ref, *scratch):
        step((idx_ref, own_ref, pair_ref), out_ref, scratch, lambda: None)

    return pl.pallas_call(
        kernel, out_shape=unpacked(idx, rec_own, heads), in_specs=[SMEM_SPEC, ANY_SPEC, ANY_SPEC], out_specs=VMEM_SPEC,
        scratch_shapes=unpack_scratch(rec_own, heads), compiler_params=local_params(), name="unpack_rows", cost_estimate=cost(16),
    )(idx, rec_own, rec_pair)


def pack_rows(pos, dst, span, grad_own, grad_pair, n_tgt):
    n = grad_own.shape[0]
    n_row = 2 * n_tgt * SLOTS
    low = I32.max

    def kernel(pos_ref, dst_ref, span_ref, own_ref, pair_ref, out_ref, g_ref, stage, sem):
        first = pltpu.make_async_copy(own_ref, g_ref.at[pl.ds(0, n)], sem.at[0])
        second = pltpu.make_async_copy(pair_ref, g_ref.at[pl.ds(n, n)], sem.at[1])
        first.start()
        second.start()
        first.wait()
        second.wait()

        begin, size = span_ref[0], span_ref[1]

        def blk(b, acc):
            base = begin + b * UNROLL
            for j in range(UNROLL):
                p = pos_ref[base + j]
                row = g_ref[pair_at(p & low), :]
                acc = row + jnp.where(jnp.full((2, LANES), p, jnp.int32) < 0, acc, 0.0)
                stage[pair_at(dst_ref[base + j]), :] = acc
            return acc

        lax.fori_loop(0, (size + UNROLL - 1) // UNROLL, blk, jnp.zeros((2, LANES), F32))
        done = pltpu.make_async_copy(stage.at[pl.ds(0, n_row)], out_ref, sem.at[0])
        done.start()
        done.wait()

    return pl.pallas_call(
        kernel, out_shape=shape_of((n_row, LANES), F32),
        in_specs=[SMEM_SPEC, SMEM_SPEC, SMEM_SPEC, ANY_SPEC, ANY_SPEC], out_specs=ANY_SPEC,
        scratch_shapes=[pltpu.VMEM((2 * n, LANES), F32), pltpu.VMEM((n_row + 8, LANES), F32), pltpu.SemaphoreType.DMA((2,))],
        compiler_params=local_params(), name="pack_rows", cost_estimate=cost(26),
    )(pos, dst, span, grad_own, grad_pair)


def owner_scatter(ids, rec, rows, place):
    n_src = rec.shape[0] // (2 * SLOTS)
    per = UNROLL

    blk_rows = 2 * rows // PLANE

    def kernel(ids_ref, place_ref, rec_ref, *refs):
        outs, (acc, buf, sem, osem) = refs[:PLANE], refs[PLANE:]
        reads = [pltpu.make_async_copy(rec_ref.at[pl.ds(s * 2 * SLOTS, 2 * SLOTS)], buf.at[pl.ds(s * 2 * SLOTS, 2 * SLOTS)], sem.at[s])
                 for s in range(n_src)]
        for c in reads:
            c.start()

        def zero(i, c):
            acc[pl.ds(i * LANES, LANES), :] = jnp.zeros((LANES, LANES), F32)
            return c

        lax.fori_loop(0, 2 * rows // LANES, zero, 0)
        for s in range(n_src):
            reads[s].wait()

            def blk(b, c):
                at = [pair_at(ids_ref[s * IDW + b * per + j]) for j in range(per)]
                base = pl.multiple_of((s * SLOTS + b * per) * 2, 2 * per)
                new = [acc[i, :] + buf[pl.ds(base + 2 * j, 2), :] for j, i in enumerate(at)]
                for i, v in zip(at, new):
                    acc[i, :] = v
                return c

            lax.fori_loop(0, SLOTS // per, blk, 0)
        writes = []
        for b in range(PLANE):
            at = pl.multiple_of((place_ref[0] ^ b) * blk_rows, blk_rows)
            writes.append(pltpu.make_async_copy(acc.at[pl.ds(at, blk_rows)], outs[b], osem.at[b]))
            writes[-1].start()
        for c in writes:
            c.wait()

    return pl.pallas_call(
        kernel, out_shape=[shape_of((blk_rows, LANES), F32)] * PLANE, in_specs=[SMEM_SPEC, SMEM_SPEC, ANY_SPEC],
        out_specs=[ANY_SPEC] * PLANE,
        scratch_shapes=[pltpu.VMEM((2 * rows + 8, LANES), F32), pltpu.VMEM((n_src * 2 * SLOTS, LANES), F32),
                        pltpu.SemaphoreType.DMA((n_src,)), pltpu.SemaphoreType.DMA((PLANE,))],
        compiler_params=local_params(), name="owner_scatter", cost_estimate=cost(20),
    )(ids, place, rec)


def finish_table(blocks, grads, which, n_tab):
    blk_rows = blocks[0].shape[0]
    blk = blk_rows // 2
    shape = (n_tab, PLANE * blk, COLS)
    first = grads is None

    def kernel(*refs):
        out, buf, stage, isem, osem = refs[-5:]
        reads = [pltpu.make_async_copy(refs[b], buf.at[b], isem.at[b]) for b in range(PLANE)]
        for c in reads:
            c.start()
        writes = []
        for b in range(PLANE):
            reads[b].wait()
            for c in range(2):
                stage[b, :, c * LANES:(c + 1) * LANES] = buf[b, pl.ds(c, blk, stride=2), :]
            writes.append(pltpu.make_async_copy(stage.at[b], out.at[which, pl.ds(b * blk, blk)], osem.at[b]))
            writes[-1].start()
        for c in writes:
            c.wait()

    args = list(blocks) + ([] if first else [grads])
    return pl.pallas_call(
        kernel, out_shape=shape_of(shape, F32), in_specs=[ANY_SPEC] * len(args), out_specs=ANY_SPEC,
        scratch_shapes=[pltpu.VMEM((PLANE, blk_rows, LANES), F32), pltpu.VMEM((PLANE, blk, COLS), F32),
                        pltpu.SemaphoreType.DMA((PLANE,)), pltpu.SemaphoreType.DMA((PLANE,))],
        input_output_aliases={} if first else {PLANE: 0},
        compiler_params=local_params(), name="finish_table", cost_estimate=cost(8))(*args)


def swap_cores(x, n_dev):
    return lax.ppermute(x, 'emb', [(i, i ^ 1) for i in range(n_dev)])


def chip_trade(x, n_dev):
    groups = [list(range(c, n_dev, 2)) for c in range(2)]
    return lax.all_to_all(x, 'emb', 0, 0, axis_index_groups=groups, tiled=True)


def chip_exchange(blocks, cid, n_chip):
    def kernel(x_ref, o_ref, ssem, rsem, lsem):
        me = lax.axis_index('emb')
        chip = me // 2
        barrier = pltpu.get_barrier_semaphore()
        for d in range(1, n_chip):
            pl.semaphore_signal(barrier, inc=1, device_id=(me ^ (2 * d),), device_id_type=MESH)
        pl.semaphore_wait(barrier, n_chip - 1)
        copies = [pltpu.make_async_copy(x_ref.at[chip], o_ref.at[chip], lsem)]
        for d in range(1, n_chip):
            copies.append(pltpu.make_async_remote_copy(
                src_ref=x_ref.at[chip ^ d], dst_ref=o_ref.at[chip], send_sem=ssem.at[d], recv_sem=rsem.at[d],
                device_id=(me ^ (2 * d),), device_id_type=MESH))
        for c in copies:
            c.start()
        for c in copies:
            c.wait()

    return pl.pallas_call(
        kernel, out_shape=shape_of(blocks.shape, blocks.dtype), in_specs=[ANY_SPEC], out_specs=ANY_SPEC,
        scratch_shapes=[pltpu.SemaphoreType.DMA((n_chip,)), pltpu.SemaphoreType.DMA((n_chip,)), pltpu.SemaphoreType.DMA],
        compiler_params=remote_params(cid), name="chip_exchange", cost_estimate=cost(100))(blocks)


def plane_trade(x, n_dev):
    groups = [list(range(z, z + PLANE)) for z in range(0, n_dev, PLANE)]
    return lax.all_to_all(x, 'emb', 0, 0, axis_index_groups=groups, tiled=True)


def empty_array(shape, dtype):
    return pl.pallas_call(lambda o: None, out_shape=shape_of(shape, dtype), out_specs=ANY_SPEC, name="empty")()


def place_trade(blocks, n_dev):
    return [blocks[0]] + [lax.ppermute(blocks[b], 'emb', [(i, i ^ b) for i in range(n_dev)]) for b in range(1, PLANE)]


def after(x, *deps):
    return lax.optimization_barrier((x,) + deps)[0]


def sort_requests(ids_pair, rows_dev, n_dev):
    n = ids_pair.shape[0]
    n_chip = n_dev // 2
    blk = rows_dev // PLANE
    owner, local = ids_pair // rows_dev, lax.rem(ids_pair, rows_dev)
    server = owner ^ (local // blk)
    name = (lax.rem(server, 2) * n_chip + server // 2) * rows_dev + lax.rem(owner, PLANE) * blk + lax.rem(local, blk)
    return lax.sort(name * n + jnp.arange(n, dtype=jnp.int32))


def route_plan(key, n_own, rows_dev, n_dev, me):
    n = key.shape[0]
    n_chip = n_dev // 2
    sid, pos = key // n, lax.rem(key, n)
    n_low = jnp.sum((sid < n_chip * rows_dev).astype(jnp.int32))
    first = sid != jnp.concatenate([jnp.full((1,), -1, jnp.int32), sid[:-1]])
    slot = jnp.cumsum(first.astype(jnp.int32)) - 1
    tgt = sid // rows_dev
    bound = jnp.arange(n_dev + 1, dtype=jnp.int32)
    start = jnp.sum((first[None, :] & (tgt[None, :] < bound[:, None])).astype(jnp.int32), axis=1)
    rank = slot - jnp.sum(jnp.where(tgt[None, :] == bound[:-1, None], start[:-1, None], 0), axis=0)
    code = tgt * (2 * rows_dev) + rank
    count = start[1:] - start[:-1]
    core = lax.rem(me, 2)
    size = jnp.where(core == 0, n_low, n - n_low)
    begin = jnp.where(core == 0, 0, n_low)
    mine = sid // (n_chip * rows_dev) == core
    marks = jnp.concatenate([start, jnp.stack([core * n_chip, jnp.max(count)])])
    return dict(pos=jnp.pad(2 * pos + jnp.where(first, 0, I32.min), (0, UNROLL)),
                code=jnp.pad(jnp.where(mine, code, -1), (0, UNROLL), constant_values=-1),
                span=jnp.stack([begin, size]), distinct=jnp.where(first & mine, sid, I32.max), marks=marks,
                by_pos=jnp.where(pos < n_own, pos * (n_dev * 2 * rows_dev) + code, I32.max))


def round_slot(code, span, rnd, trash, width):
    tgt, rank = code // span, lax.rem(code, span) - rnd * SLOTS
    inside = (code >= 0) & (rank >= 0) & (rank < SLOTS)
    return jnp.where(inside, tgt * width + rank, trash)


def solution(mesh):
    n_dev = mesh.shape['emb']
    n_chip = n_dev // 2
    tok_spec = P('emb', None)
    tab_spec = P(None, 'emb', None)

    def step(x_start, d_out, token_ids, w_up, w_down, w_gate, w_proj, tables):
        n_tab, n_tok, n_heads = token_ids.shape
        rows_dev, row_width = tables.shape[1], tables.shape[2]
        n_req = n_tok * n_heads
        tail = (row_width // LANES, LANES)
        me = lax.axis_index('emb')
        core = lax.rem(me, 2)

        flat_ids = token_ids.reshape(n_tab, n_req)
        ids_pair = jnp.concatenate([flat_ids, swap_cores(flat_ids, n_dev)], axis=1)
        place = lax.rem(me, PLANE).reshape(1)
        split = split_rows(tables, place)
        served = plane_trade(split, n_dev)
        keys = [sort_requests(after(ids_pair, split)[t], rows_dev, n_dev) for t in range(n_tab)]

        plans = [route_plan(keys[t], n_req, rows_dev, n_dev, me) for t in range(n_tab)]
        distinct = lax.sort(jnp.stack([plan['distinct'] for plan in plans]), dimension=1)
        x1 = layer_plain(after(x_start, *[plan['distinct'] for plan in plans]), w_up, w_down, 0)
        distinct = distinct.reshape(n_tab, -1, 1, LANES)
        span = 2 * rows_dev
        in_order = lax.sort(after(jnp.stack([plan['by_pos'] for plan in plans]), distinct), dimension=1)
        code_own = lax.rem(in_order[:, :n_req], n_dev * span)

        def half_slot(plan, rnd, width, trash):
            code = plan['code']
            code = jnp.where(code >= 0, lax.rem(code, n_chip * span), code)
            return round_slot(code, span, rnd, trash, width)

        def id_blocks(tabs, rnd):
            marks = jnp.concatenate([plans[t]['marks'] for t in tabs])
            return make_ids(distinct[tabs[0]:tabs[-1] + 1], marks, rnd, rows_dev)

        blocks = id_blocks(range(n_tab), jnp.int32(0))
        got = chip_exchange(after(blocks, served, x1), 9, n_chip).reshape(n_chip, n_tab, IDW)
        first_ids = [got[:, t].reshape(n_chip * IDW) for t in range(n_tab)]
        rounds = [(jnp.max(got[:, t, IDW - 1]) + SLOTS - 1) // SLOTS for t in range(n_tab)]

        def more_ids(which, rnd, cid):
            return chip_exchange(id_blocks([which], rnd), cid, n_chip).reshape(n_chip * IDW)

        def own_slot(which, rnd):
            half = n_chip * SLOTS
            slot = round_slot(code_own[which], span, rnd, 2 * half, SLOTS)
            return jnp.where((core == 0) | (slot == 2 * half), slot, lax.rem(slot + half, 2 * half))

        def unpack(which, rnd, own):
            return unpack_rows(own_slot(which, rnd), own, swap_cores(own, n_dev), n_heads)

        def late_rows(start):
            def more(state):
                rnd, now = state[0], []
                for t in range(n_tab):
                    sent = owner_gather(more_ids(t, rnd, t), served, t, n_chip).reshape((n_chip, SLOTS) + tail)
                    new = unpack(t, rnd, chip_exchange(sent, 2 + t, n_chip).reshape((n_chip * SLOTS,) + tail))
                    mine = lax.rem(code_own[t], span) // SLOTS == rnd
                    now.append(jnp.where(jnp.repeat(mine, row_width).reshape(new.shape), new, state[1 + t]))
                return (rnd + 1, *now)

            most = jnp.maximum(*rounds)

            def nothing():
                return tuple(empty_array((n_tok, n_heads * row_width), BF16) for _ in range(n_tab))

            def loop():
                return lax.while_loop(lambda s: s[0] < most, more, (jnp.int32(1), *nothing()))[1:]

            return lax.cond(after(most, *start) > 1, loop, nothing)

        def parts(which, own):
            return own_slot(which, 0), own, swap_cores(own, n_dev), late[which], rounds[which].reshape(1)

        def packed(which, rnd, grad_own, grad_pair):
            plan = plans[which]
            dst = 2 * half_slot(plan, rnd, SLOTS, n_chip * SLOTS)
            return pack_rows(plan['pos'], dst, plan['span'], grad_own, grad_pair, n_chip)

        def return_rest(which, first, pair):
            def more(state):
                rnd, total = state
                ids = more_ids(which, rnd, 4 + which)
                rec = chip_exchange(packed(which, rnd, *pair).reshape(n_chip, 2 * SLOTS, LANES), 6 + which, n_chip)
                new = owner_scatter(ids, rec.reshape(n_chip * 2 * SLOTS, LANES), rows_dev, place)
                return rnd + 1, [p + q for p, q in zip(total, new)]

            return lax.while_loop(lambda s: s[0] < rounds[which], more, (jnp.int32(1), list(first)))[1]

        sent0 = owner_gather(first_ids[0], served, 0, n_chip)
        fetched0 = chip_trade(sent0, n_dev)
        m1, g1, sent1 = layer_table_head(after(x1, sent0), w_up, w_down, w_gate, 1, 0, first_ids[1], served, n_chip)
        late = late_rows((m1, fetched0))
        rows0 = parts(0, after(fetched0, *late))
        fetched1 = chip_trade(after(sent1, fetched0, *late), n_dev)
        x2, h2, x3, a3, dz3, rows3 = layer_middle(x1, m1, g1, rows0, d_out, w_up, w_down, w_gate, w_proj, 2, n_heads)
        pair1 = rows3, swap_cores(rows3, n_dev)
        h3 = last_up(x3, w_up, 3)
        rows1 = parts(1, after(fetched1, h3))
        sent1 = packed(1, 0, pair1[0], after(pair1[1], h3))
        returned1 = chip_trade(after(sent1, fetched1), n_dev)
        c2, e3 = back_table(after(d_out, sent1), h3, x3, a3, dz3, rows1, w_up, w_down, w_gate, 3, 1, n_heads)
        pair0 = back_plain(c2, h2, x2, g1, w_up, w_down, w_proj, 2, 0)
        sent0 = packed(0, 0, *pair0)
        returned0 = chip_trade(after(sent0, returned1), n_dev)
        total1 = owner_scatter(first_ids[1], after(returned1, sent0), rows_dev, place)
        total1 = return_rest(1, total1, pair1)
        placed1 = place_trade(total1, n_dev)
        x_end = last_down(after(x3, *total1), h3, a3, e3, w_down, w_proj, 3, 1)
        total0 = owner_scatter(first_ids[0], after(returned0, x_end), rows_dev, place)
        total0 = return_rest(0, total0, pair0)
        placed0 = place_trade(total0, n_dev)
        grads = finish_table([after(p, *total0) for p in placed1], None, 1, n_tab)
        grads = finish_table(placed0, grads, 0, n_tab)
        return x_end, grads

    return jax.shard_map(step, mesh=mesh, in_specs=(tok_spec, tok_spec, tab_spec, P(), P(), P(), P(), tab_spec),
                         out_specs=(tok_spec, tab_spec), check_vma=False)
```
